8 devices in a mesh: rep: 2 (over z, y), blk: 4 (over x, core).
Axes of the slice: x: 2, y: 2, z: 1, core: 2. Of those that a mesh axis runs over, the one named last changes fastest.
Arguments:
- ratings: float32 [512, 4096], P(None, ('rep', 'blk')), parts along dimension 1
- observed: int32 [512, 4096], P(None, ('rep', 'blk')), parts along dimension 1
- user_init: float32 [1024, 50], P(('rep', 'blk')), parts along dimension 0
- item_init: float32 [4096, 50], P(('rep', 'blk')), parts along dimension 0
- lr_scale: float32 [64, 4], replicated
Outputs:
- output 1: float32 [1024, 50], P(('rep', 'blk')), parts along dimension 0
- output 2: float32 [4096, 50], P(('rep', 'blk')), parts along dimension 0
There are 2 independent parts. The reference program is written for one: setup_inputs(seed, part) draws one part's arguments, and reference() takes and returns one part's arrays. A program takes and returns all parts, laid end to end along the dimension named above; an argument that names none is the same for every part.
All inputs are finite; a program needn't handle non-finite values.
Results may differ from the reference program's by a relative error of at most 0.001.
Values are sent between devices in bfloat16 or wider.
A program may use at most 1 GiB of HBM per device.

```python
import math
import jax
import jax.numpy as jnp
from jax import lax

USERS = 512
COLS_DEV = 512
RANK = 50
NUM_BLOCKS = 4
STEPS = 4
EPOCHS = 16
NUM_ITEMS = NUM_BLOCKS * COLS_DEV
BLOCK_ROWS = USERS // NUM_BLOCKS
STEP_BASE = math.sqrt(RANK) / (4.0 * (COLS_DEV + 2 * RANK))
LAMBDA = 0.05
INIT_SCALE = RANK ** -0.25


def setup_inputs(seed: int = 0, part: int = 0) -> dict:
    base_key = jax.random.key(seed)
    shared_key, part_root = jax.random.split(base_key)
    part_key = jax.random.fold_in(part_root, part)
    key_list = jax.random.split(part_key, 7)
    left_true = jax.random.normal(key_list[0], (USERS, RANK), jnp.float32) * INIT_SCALE
    right_true = jax.random.normal(key_list[1], (NUM_ITEMS, RANK), jnp.float32) * INIT_SCALE
    noise_draw = jax.random.normal(key_list[2], (USERS, NUM_ITEMS), jnp.float32)
    ratings = jnp.dot(left_true, right_true.T) + 0.3 * noise_draw
    row_pct = jax.random.randint(key_list[3], (USERS, 1), 10, 41)
    pct_draws = jax.random.randint(key_list[4], (USERS, NUM_ITEMS), 0, 100)
    observed = (pct_draws < row_pct).astype(jnp.int32)
    user_init = jax.random.normal(key_list[5], (USERS, RANK), jnp.float32) * INIT_SCALE
    item_init = jax.random.normal(key_list[6], (NUM_ITEMS, RANK), jnp.float32) * INIT_SCALE
    lr_scale = jax.random.uniform(shared_key, (EPOCHS * NUM_BLOCKS, STEPS), jnp.float32, 0.25, 1.0)
    return {"ratings": ratings, "observed": observed, "user_init": user_init, "item_init": item_init, "lr_scale": lr_scale}


def as_bf16_values(values):
    return values.astype(jnp.bfloat16).astype(jnp.float32)


def reference(ratings, observed, user_init, item_init, lr_scale):
    rate_grid = ratings.reshape(NUM_BLOCKS, BLOCK_ROWS, NUM_BLOCKS, COLS_DEV)
    mask_grid = observed.astype(jnp.float32).reshape(NUM_BLOCKS, BLOCK_ROWS, NUM_BLOCKS, COLS_DEV)
    item_ids = jnp.arange(NUM_BLOCKS)

    def sub_epoch(carry, step_inputs):
        user_blocks, item_blocks = carry
        t_index, scales = step_inputs
        user_ids = (item_ids + t_index) % NUM_BLOCKS
        rate_now = rate_grid[user_ids, :, item_ids, :]
        mask_now = mask_grid[user_ids, :, item_ids, :]

        def one_step(step_state, scale_val):
            users_cur, items_cur = step_state
            users_bf = as_bf16_values(users_cur)
            items_bf = as_bf16_values(items_cur)
            approx = jnp.einsum("jar,jbr->jab", users_bf, items_bf)
            errors = as_bf16_values(mask_now * (approx - rate_now))
            grad_u = jnp.einsum("jab,jbr->jar", errors, items_bf) + LAMBDA * users_cur
            grad_v = jnp.einsum("jab,jar->jbr", errors, users_bf) + LAMBDA * items_cur
            step_size = STEP_BASE * scale_val
            return (users_cur - step_size * grad_u, items_cur - step_size * grad_v), None

        (users_new, items_new), _ = lax.scan(one_step, (user_blocks[user_ids], item_blocks), scales)
        home_ids = (item_ids - t_index) % NUM_BLOCKS
        return (users_new[home_ids], items_new), None

    user_blocks = user_init.reshape(NUM_BLOCKS, BLOCK_ROWS, RANK)
    item_blocks = item_init.reshape(NUM_BLOCKS, COLS_DEV, RANK)
    t_values = jnp.arange(EPOCHS * NUM_BLOCKS) % NUM_BLOCKS
    (user_blocks, item_blocks), _ = lax.scan(sub_epoch, (user_blocks, item_blocks), (t_values, lr_scale))
    return user_blocks.reshape(USERS, RANK), item_blocks.reshape(NUM_ITEMS, RANK)
```

```python
import functools
import math

import jax
import jax.numpy as jnp
from jax import lax
from jax.experimental import pallas as pl
from jax.experimental.pallas import tpu as pltpu
from jax.sharding import PartitionSpec as P

LAMBDA = 0.05
LEADER = 1
STEPS = 4
KPAD = 64
F32 = jnp.float32
BF16 = jnp.bfloat16
MESH_ID = pl.DeviceIdType.MESH


def make_order(nb, subs, len_a=64, len_b=96, a_to_b=226, b_to_c=211, len_c=56):
    def deps(s, i):
        if s == 0:
            return []
        return [(s - 1, i)] + ([(s - 1, (i - 1) % nb)] if s % STEPS == 0 else [])

    todo_a = {(s, i) for s in range(STEPS * subs) for i in range(nb)}
    todo_b, start_a, done_c, events, now = set(), {}, {}, [], 0
    while todo_a or todo_b:
        cand = []
        first = min((s for s, _ in todo_a), default=0)
        for s, i in todo_a:
            if s <= first + 1 and all(d in done_c for d in deps(s, i)):
                ready = max([done_c[d] for d in deps(s, i)], default=0)
                cand.append((max(ready, now), s * 10 + 5, nb - i, "A", s, i))
        for s, i in todo_b:
            cand.append((max(start_a[s, i] + a_to_b, now), s * 10, nb - i, "B", s, i))
        begin, _, _, kind, s, i = min(cand)
        if kind == "A":
            start_a[s, i] = begin
            todo_a.remove((s, i))
            todo_b.add((s, i))
            now = begin + len_a
            events.append((begin, 0, kind, s, i))
        else:
            todo_b.remove((s, i))
            now = begin + len_b
            done_c[s, i] = now + b_to_c + len_c
            events.append((begin, 1, kind, s, i))
            events.append((now + b_to_c, 2, "C", s, i))
    return [e[2:] for e in sorted(events)]


def dot(a, b):
    return jnp.dot(a, b, preferred_element_type=F32)


def dot_nt(a, b):
    return lax.dot_general(a, b, (((1,), (1,)), ((), ())), preferred_element_type=F32)


def kernel(nb, rank, base_eta, lr, rate, ut_in, vt_in, ut_out, vt_out,
           r_all, m_all, ut_land, vt_land, u32, v32, ub, utb, vb,
           r_sem, s_sem, u_sem, v_sem, us_sem, vs_sem, ou_sem, ov_sem, ous_sem, ovs_sem):
    me = lax.axis_index("blk")
    rows = r_all.shape[2]
    subs = lr.shape[0]
    barrier = pltpu.get_barrier_semaphore()

    def block_copy(w):
        start = pl.multiple_of(lax.rem(me + w, nb) * rows, rows)
        return rate.at[pl.ds(start, rows)]

    @pl.when(me != LEADER)
    def _():
        pl.semaphore_signal(barrier, inc=1, device_id={"blk": LEADER}, device_id_type=MESH_ID)
        pl.semaphore_wait(barrier, 1)
        to = dict(device_id={"blk": LEADER}, device_id_type=MESH_ID)
        cps = [
            pltpu.make_async_remote_copy(ut_in, ut_land.at[me], us_sem, u_sem.at[me], **to),
            pltpu.make_async_remote_copy(vt_in, vt_land.at[me], vs_sem, v_sem.at[me], **to),
        ]
        for w in range(nb):
            cps.append(pltpu.make_async_remote_copy(block_copy(w), r_all.at[w, me], s_sem.at[w], r_sem.at[w, me], **to))
        for cp in cps:
            cp.start()
        for cp in cps:
            cp.wait_send()
        pltpu.make_async_copy(ut_out, ut_out, ou_sem).wait()
        pltpu.make_async_copy(vt_out, vt_out, ov_sem).wait()

    @pl.when(me == LEADER)
    def _():
        others = [j for j in range(nb) if j != LEADER]
        for j in others:
            pl.semaphore_signal(barrier, inc=1, device_id={"blk": j}, device_id_type=MESH_ID)
        pl.semaphore_wait(barrier, nb - 1)
        pltpu.make_async_copy(ut_in, ut_land.at[LEADER], u_sem.at[LEADER]).start()
        pltpu.make_async_copy(vt_in, vt_land.at[LEADER], v_sem.at[LEADER]).start()
        for w in range(nb):
            pltpu.make_async_copy(block_copy(w), r_all.at[w, LEADER], r_sem.at[w, LEADER]).start()

        for i in range(nb):
            pltpu.make_async_copy(ut_land.at[i], ut_land.at[i], u_sem.at[i]).wait()
            pltpu.make_async_copy(vt_land.at[i], vt_land.at[i], v_sem.at[i]).wait()
            v32[i] = jnp.zeros(v32.shape[1:], F32)
            v32[i, :rank] = vt_land[i]
            vb[i] = v32[i].astype(BF16)
            ut = jnp.concatenate([ut_land[i], jnp.zeros((rows - rank, rows), F32)], axis=0)
            u32[i] = ut.T[:, :KPAD]
            ub[i] = ut.T[:, :KPAD].astype(BF16)
            utb[i] = ut[:KPAD].astype(BF16)

        def run(order, t0, w_of, j_of):
            prod, gu, gv = {}, {}, {}
            for kind, s, i in order:
                sub = s // STEPS
                j, w = j_of(sub, i), w_of(sub)
                if kind == "A":
                    prod[s, i] = dot(ub[i], vb[j])
                elif kind == "B":
                    err = (prod.pop((s, i)) - r_all[w, j]).astype(BF16) * m_all[w, j]
                    gu[s, i] = dot_nt(err, vb[j])
                    gv[s, i] = dot(utb[i], err)
                else:
                    eta = lr[t0 + sub, s % STEPS] * base_eta
                    keep = 1.0 - eta * LAMBDA
                    u_new = u32[i] * keep - eta * gu.pop((s, i))
                    u32[i] = u_new
                    u_bf = u_new.astype(BF16)
                    ub[i] = u_bf
                    utb[i] = u_bf.T
                    v_new = v32[j] * keep - eta * gv.pop((s, i))
                    v32[j] = v_new
                    vb[j] = v_new.astype(BF16)

        order_1 = make_order(nb, 1)
        order_n = make_order(nb, nb)

        def first_epoch(w, carry):
            for j in range(nb):
                pltpu.make_async_copy(r_all.at[w, j], r_all.at[w, j], r_sem.at[w, j]).wait()
                coded = r_all[w, j]
                seen = coded < jnp.inf
                m_all[w, j] = jnp.where(seen, 1.0, 0.0).astype(BF16)
                r_all[w, j] = jnp.where(seen, coded, 0.0)
            run(order_1, w, lambda sub: w, lambda sub, i: lax.rem(i - w + nb, nb))
            return carry

        def epoch(e, carry):
            run(order_n, e * nb, lambda sub: sub, lambda sub, i: (i - sub) % nb)
            return carry

        lax.fori_loop(0, nb, first_epoch, 0)
        lax.fori_loop(1, subs // nb, epoch, 0)

        for i in range(nb):
            ut = jnp.concatenate([u32[i], jnp.zeros((rows, rows - KPAD), F32)], axis=1).T
            ut_land[i] = ut[:rank]
            vt_land[i] = v32[i, :rank]
        cps = []
        for n, j in enumerate(others):
            to = dict(device_id={"blk": j}, device_id_type=MESH_ID)
            cps.append(pltpu.make_async_remote_copy(vt_land.at[j], vt_out, ovs_sem.at[n], ov_sem, **to))
            cps.append(pltpu.make_async_remote_copy(ut_land.at[j], ut_out, ous_sem.at[n], ou_sem, **to))
        for cp in cps:
            cp.start()
        ut_out[...] = ut_land[LEADER]
        vt_out[...] = vt_land[LEADER]
        for cp in cps:
            cp.wait_send()


def solution(mesh):
    nb = mesh.shape["blk"]

    def local_run(rate_loc, mask_loc, user_loc, item_loc, lr_scale):
        rows, rank = user_loc.shape
        cols = item_loc.shape[0]
        base_eta = math.sqrt(rank) / (4.0 * (cols + 2 * rank))
        coded = jnp.where(mask_loc != 0, rate_loc, jnp.inf)
        vmem = pl.BlockSpec(memory_space=pltpu.VMEM)
        dma = pltpu.SemaphoreType.DMA
        ut, vt = pl.pallas_call(
            functools.partial(kernel, nb, rank, base_eta),
            out_shape=(jax.ShapeDtypeStruct((rank, rows), F32), jax.ShapeDtypeStruct((rank, cols), F32)),
            in_specs=[pl.BlockSpec(memory_space=pltpu.SMEM), pl.BlockSpec(memory_space=pl.ANY), vmem, vmem],
            out_specs=(vmem, vmem),
            scratch_shapes=[
                pltpu.VMEM((nb, nb, rows, cols), F32),
                pltpu.VMEM((nb, nb, rows, cols), BF16),
                pltpu.VMEM((nb, rank, rows), F32),
                pltpu.VMEM((nb, rank, cols), F32),
                pltpu.VMEM((nb, rows, KPAD), F32),
                pltpu.VMEM((nb, KPAD, cols), F32),
                pltpu.VMEM((nb, rows, KPAD), BF16),
                pltpu.VMEM((nb, KPAD, rows), BF16),
                pltpu.VMEM((nb, KPAD, cols), BF16),
                dma((nb, nb)), dma((nb,)), dma((nb,)), dma((nb,)), dma, dma,
                dma, dma, dma((nb - 1,)), dma((nb - 1,)),
            ],
            compiler_params=pltpu.CompilerParams(collective_id=0, has_side_effects=True),
            name="dsgd",
        )(lr_scale, coded, user_loc.T, item_loc.T)
        return ut.T, vt.T

    spec_cols = P(None, ("rep", "blk"))
    spec_rows = P(("rep", "blk"), None)
    return jax.shard_map(
        local_run,
        mesh=mesh,
        in_specs=(spec_cols, spec_cols, spec_rows, spec_rows, P(None, None)),
        out_specs=(spec_rows, spec_rows),
        check_vma=False,
    )
```

```python
import functools
import math
import random

import jax
import jax.numpy as jnp
from jax import lax
from jax.experimental import pallas as pl
from jax.experimental.pallas import tpu as pltpu
from jax.sharding import PartitionSpec as P

LAMBDA = 0.05
LEADER = 1
STEPS = 4
KPAD = 64
UNROLL = 12
LEN_A, LEN_B, A_TO_B, B_TO_C, LEN_C = 64, 96, 226, 211, 80
F32 = jnp.float32
BF16 = jnp.bfloat16
MESH_ID = pl.DeviceIdType.MESH


def play(order, nb):
    now, start, done = 0, {}, {}
    for kind, s, i in order:
        if kind == "A":
            ready = 0
            if s > 0:
                before = [(s - 1, i)] + ([(s - 1, (i - 1) % nb)] if s % STEPS == 0 else [])
                if any(d not in done for d in before):
                    return None
                ready = max(done[d] for d in before)
            start[kind, s, i] = max(now, ready)
            now = start[kind, s, i] + LEN_A
        else:
            if ("A", s, i) not in start:
                return None
            start[kind, s, i] = max(now, start["A", s, i] + A_TO_B)
            now = start[kind, s, i] + LEN_B
            done[s, i] = now + B_TO_C + LEN_C
    return max(done.values()), start


def make_order(nb, subs, tries):
    users = [(s, i) for s in range(STEPS * subs) for i in reversed(range(nb))]
    best = []
    for n in range(len(users) + 1):
        best += [("A", *users[n])] if n < len(users) else []
        best += [("B", *users[n - 1])] if n > 0 else []
    rnd = random.Random(0)
    cur, length = best, play(best, nb)[0]
    low = length
    for it in range(tries):
        new = list(cur)
        at = rnd.randrange(len(new))
        item = new.pop(at)
        new.insert(max(0, at + rnd.choice((-4, -3, -2, -1, 1, 2, 3, 4))), item)
        played = play(new, nb)
        if played is None:
            continue
        temp = 60 * (1 - it / tries) + 0.5
        if played[0] <= length or rnd.random() < math.exp((length - played[0]) / temp):
            cur, length = new, played[0]
            if length < low:
                best, low = new, length
    start = play(best, nb)[1]
    events = [(t, 1, *key) for key, t in start.items()]
    events += [(t + LEN_B + B_TO_C, 0, "C", s, i) for (kind, s, i), t in start.items() if kind == "B"]
    return [e[2:] for e in sorted(events)]


def dot(a, b):
    return jnp.dot(a, b, preferred_element_type=F32)


def dot_nt(a, b):
    return lax.dot_general(a, b, (((1,), (1,)), ((), ())), preferred_element_type=F32)


def kernel(nb, rank, base_eta, lr, rate, mask, ut_in, vt_in, ut_out, vt_out,
           r_all, m_all, r_own, m_own, ut_land, vt_land, u32, v32, ub, utb, vb,
           rl_sem, ml_sem, r_sem, s_sem, u_sem, v_sem, us_sem, vs_sem, ou_sem, ov_sem, ous_sem, ovs_sem):
    me = lax.axis_index("blk")
    rows, cols = r_all.shape[2:]
    subs = lr.shape[1]
    half = cols // 2
    halves = [slice(h * half, (h + 1) * half) for h in range(2)]
    barrier = pltpu.get_barrier_semaphore()

    loads = []
    for w in range(nb):
        start = pl.multiple_of(lax.rem(me + w, nb) * rows, rows)
        loads.append((
            pltpu.make_async_copy(rate.at[pl.ds(start, rows)], r_own.at[w], rl_sem.at[w]),
            pltpu.make_async_copy(mask.at[pl.ds(start, rows)], m_own.at[w], ml_sem.at[w]),
        ))
    for pair in loads:
        for cp in pair:
            cp.start()

    @pl.when(me != LEADER)
    def _():
        to = dict(device_id={"blk": LEADER}, device_id_type=MESH_ID)
        pl.semaphore_signal(barrier, inc=1, **to)

        def encode(w):
            for cp in loads[w]:
                cp.wait()
            r_own[w] = jnp.where(m_own[w] != 0, r_own[w], jnp.inf)

        encode(0)
        encode(1)
        pl.semaphore_wait(barrier, 1)
        cps = [
            pltpu.make_async_remote_copy(ut_in, ut_land.at[me], us_sem, u_sem.at[me], **to),
            pltpu.make_async_remote_copy(vt_in, vt_land.at[me], vs_sem, v_sem.at[me], **to),
        ]
        for w in range(nb):
            cps.append(pltpu.make_async_remote_copy(r_own.at[w], r_all.at[w, me], s_sem.at[w], r_sem.at[w, me], **to))
        for cp in cps[:3]:
            cp.start()
        encode(2)
        cps[3].start()
        encode(3)
        for cp in cps[4:]:
            cp.start()
        for cp in cps:
            cp.wait_send()
        pltpu.make_async_copy(ut_out, ut_out, ou_sem).wait()
        pltpu.make_async_copy(vt_out, vt_out, ov_sem).wait()

    @pl.when(me == LEADER)
    def _():
        others = [j for j in range(nb) if j != LEADER]
        for j in others:
            pl.semaphore_signal(barrier, inc=1, device_id={"blk": j}, device_id_type=MESH_ID)
        ut_land[LEADER] = ut_in[...]
        vt_land[LEADER] = vt_in[...]
        for w in range(nb):
            for cp in loads[w]:
                cp.wait()
            m_all[w, LEADER] = m_own[w].astype(F32).astype(BF16)
            r_all[w, LEADER] = r_own[w]
        pl.semaphore_wait(barrier, nb - 1)

        for i in range(nb):
            if i != LEADER:
                pltpu.make_async_copy(ut_land.at[i], ut_land.at[i], u_sem.at[i]).wait()
                pltpu.make_async_copy(vt_land.at[i], vt_land.at[i], v_sem.at[i]).wait()
            v32[i] = jnp.zeros(v32.shape[1:], F32)
            v32[i, :rank] = vt_land[i]
            vb[i] = v32[i].astype(BF16)
            ut = jnp.concatenate([ut_land[i], jnp.zeros((rows - rank, rows), F32)], axis=0)
            u32[i] = ut.T[:, :KPAD]
            ub[i] = ut.T[:, :KPAD].astype(BF16)
            utb[i] = ut[:KPAD].astype(BF16)

        def run(order, t0, w_of, j_of):
            prod, grads = {}, {}
            for kind, s, i in order:
                sub = s // STEPS
                j, w = j_of(sub, i), w_of(sub)
                if kind == "A":
                    prod[s, i] = [dot(ub[i], vb[j, :, h]) for h in halves]
                elif kind == "B":
                    errs = [
                        (a - r_all[w, j, :, h]).astype(BF16) * m_all[w, j, :, h]
                        for a, h in zip(prod.pop((s, i)), halves)
                    ]
                    gu = [dot_nt(err, vb[j, :, h]) for err, h in zip(errs, halves)]
                    grads[s, i] = gu, [dot(utb[i], err) for err in errs]
                else:
                    eta = lr[s % STEPS, t0 + sub] * base_eta
                    keep = 1.0 - eta * LAMBDA
                    gu, gv = grads.pop((s, i))
                    u_new = u32[i] * keep - eta * gu[0] - eta * gu[1]
                    u32[i] = u_new
                    u_bf = u_new.astype(BF16)
                    ub[i] = u_bf
                    utb[i] = u_bf.T
                    for g, h in zip(gv, halves):
                        v_new = v32[j, :, h] * keep - eta * g
                        v32[j, :, h] = v_new
                        vb[j, :, h] = v_new.astype(BF16)

        order_1 = make_order(nb, 1, 3000)
        order_n = make_order(nb, UNROLL, 0)

        def first_epoch(w, carry):
            for j in [j for j in range(nb) if j != LEADER]:
                pltpu.make_async_copy(r_all.at[w, j], r_all.at[w, j], r_sem.at[w, j]).wait()
                coded = r_all[w, j]
                seen = coded < jnp.inf
                m_all[w, j] = jnp.where(seen, 1.0, 0.0).astype(BF16)
                r_all[w, j] = jnp.where(seen, coded, 0.0)
            run(order_1, w, lambda sub: w, lambda sub, i: lax.rem(i - w + nb, nb))
            return carry

        def later(n, carry):
            run(order_n, nb + n * UNROLL, lambda sub: sub % nb, lambda sub, i: (i - sub) % nb)
            return carry

        lax.fori_loop(0, nb, first_epoch, 0)
        lax.fori_loop(0, (subs - nb) // UNROLL, later, 0)

        for i in range(nb):
            ut = jnp.concatenate([u32[i], jnp.zeros((rows, rows - KPAD), F32)], axis=1).T
            ut_land[i] = ut[:rank]
            vt_land[i] = v32[i, :rank]
        cps = []
        for n, j in enumerate(others):
            to = dict(device_id={"blk": j}, device_id_type=MESH_ID)
            cps.append(pltpu.make_async_remote_copy(vt_land.at[j], vt_out, ovs_sem.at[n], ov_sem, **to))
            cps.append(pltpu.make_async_remote_copy(ut_land.at[j], ut_out, ous_sem.at[n], ou_sem, **to))
        cps.reverse()
        for cp in cps:
            cp.start()
        mine = [
            pltpu.make_async_copy(ut_land.at[LEADER], ut_out, ou_sem),
            pltpu.make_async_copy(vt_land.at[LEADER], vt_out, ov_sem),
        ]
        for cp in mine:
            cp.start()
        for cp in mine:
            cp.wait()
        for cp in cps:
            cp.wait_send()


def solution(mesh):
    nb = mesh.shape["blk"]

    def local_run(rate_loc, mask_loc, user_loc, item_loc, lr_scale):
        rows, rank = user_loc.shape
        cols = item_loc.shape[0]
        base_eta = math.sqrt(rank) / (4.0 * (cols + 2 * rank))
        vmem = pl.BlockSpec(memory_space=pltpu.VMEM)
        hbm = pl.BlockSpec(memory_space=pl.ANY)
        dma = pltpu.SemaphoreType.DMA
        ut, vt = pl.pallas_call(
            functools.partial(kernel, nb, rank, base_eta),
            out_shape=(jax.ShapeDtypeStruct((rank, rows), F32), jax.ShapeDtypeStruct((rank, cols), F32)),
            in_specs=[pl.BlockSpec(memory_space=pltpu.SMEM), hbm, hbm, vmem, vmem],
            out_specs=(hbm, hbm),
            scratch_shapes=[
                pltpu.VMEM((nb, nb, rows, cols), F32),
                pltpu.VMEM((nb, nb, rows, cols), BF16),
                pltpu.VMEM((nb, rows, cols), F32),
                pltpu.VMEM((nb, rows, cols), jnp.int32),
                pltpu.VMEM((nb, rank, rows), F32),
                pltpu.VMEM((nb, rank, cols), F32),
                pltpu.VMEM((nb, rows, KPAD), F32),
                pltpu.VMEM((nb, KPAD, cols), F32),
                pltpu.VMEM((nb, rows, KPAD), BF16),
                pltpu.VMEM((nb, KPAD, rows), BF16),
                pltpu.VMEM((nb, KPAD, cols), BF16),
                dma((nb,)), dma((nb,)),
                dma((nb, nb)), dma((nb,)), dma((nb,)), dma((nb,)), dma, dma,
                dma, dma, dma((nb - 1,)), dma((nb - 1,)),
            ],
            compiler_params=pltpu.CompilerParams(collective_id=0, has_side_effects=True),
            name="dsgd",
        )(lr_scale.T, rate_loc, mask_loc, user_loc.T, item_loc.T)
        return ut.T, vt.T

    spec_cols = P(None, ("rep", "blk"))
    spec_rows = P(("rep", "blk"), None)
    return jax.shard_map(
        local_run,
        mesh=mesh,
        in_specs=(spec_cols, spec_cols, spec_rows, spec_rows, P(None, None)),
        out_specs=(spec_rows, spec_rows),
        check_vma=False,
    )
```

```python
import functools
import math
import random

import jax
import jax.numpy as jnp
from jax import lax
from jax.experimental import pallas as pl
from jax.experimental.pallas import tpu as pltpu
from jax.sharding import PartitionSpec as P

LAMBDA = 0.05
STEPS = 4
KPAD = 64
UNROLL = 12
LEN_A, LEN_B, A_TO_B, B_TO_C, LEN_C = 64, 96, 226, 211, 80
F32 = jnp.float32
BF16 = jnp.bfloat16
MESH_ID = pl.DeviceIdType.MESH


def play(order, nb):
    now, start, done = 0, {}, {}
    for kind, s, i in order:
        if kind == "A":
            ready = 0
            if s > 0:
                before = [(s - 1, i)] + ([(s - 1, (i - 1) % nb)] if s % STEPS == 0 else [])
                if any(d not in done for d in before):
                    return None
                ready = max(done[d] for d in before)
            start[kind, s, i] = max(now, ready)
            now = start[kind, s, i] + LEN_A
        else:
            if ("A", s, i) not in start:
                return None
            start[kind, s, i] = max(now, start["A", s, i] + A_TO_B)
            now = start[kind, s, i] + LEN_B
            done[s, i] = now + B_TO_C + LEN_C
    return max(done.values()), start


def make_order(nb, subs, tries):
    users = [(s, i) for s in range(STEPS * subs) for i in reversed(range(nb))]
    best = []
    for n in range(len(users) + 1):
        best += [("A", *users[n])] if n < len(users) else []
        best += [("B", *users[n - 1])] if n > 0 else []
    rnd = random.Random(0)
    cur, length = best, play(best, nb)[0]
    low = length
    for it in range(tries):
        new = list(cur)
        at = rnd.randrange(len(new))
        item = new.pop(at)
        new.insert(max(0, at + rnd.choice((-4, -3, -2, -1, 1, 2, 3, 4))), item)
        played = play(new, nb)
        if played is None:
            continue
        temp = 60 * (1 - it / tries) + 0.5
        if played[0] <= length or rnd.random() < math.exp((length - played[0]) / temp):
            cur, length = new, played[0]
            if length < low:
                best, low = new, length
    start = play(best, nb)[1]
    events = [(t, 1, *key) for key, t in start.items()]
    events += [(t + LEN_B + B_TO_C, 0, "C", s, i) for (kind, s, i), t in start.items() if kind == "B"]
    return [e[2:] for e in sorted(events)]


def dot(a, b):
    return jnp.dot(a, b, preferred_element_type=F32)


def dot_nt(a, b):
    return lax.dot_general(a, b, (((1,), (1,)), ((), ())), preferred_element_type=F32)


def kernel(nb, rank, base_eta, lr, rate, mask, ut_in, vt_in, ut_out, vt_out,
           r_all, m_all, r_own, m_own, hop_1, hop_2, ut_land, vt_land, u32, v32, ub, utb, vb,
           rl_sem, ml_sem, r_sem, s_sem, u_sem, v_sem, us_sem, vs_sem, ou_sem, ov_sem, ous_sem, ovs_sem,
           h1_sem, h1s_sem, h2_sem, h2s_sem, h3_sem, h3s_sem):
    me = lax.axis_index("blk")
    rep = lax.axis_index("rep")
    other = 1 - rep
    lead = 2 * rep + 1
    mate = 2 * rep
    far_0 = lax.rem(lead + 1, nb)
    far_1 = lax.rem(lead + 2, nb)
    late = nb - 1
    parts = hop_1.shape[1]
    rows, cols = r_all.shape[2:]
    subs = lr.shape[1]
    half = cols // 2
    halves = [slice(h * half, (h + 1) * half) for h in range(2)]
    barrier = pltpu.get_barrier_semaphore()

    loads = []
    for w in range(nb):
        start = pl.multiple_of(lax.rem(me + w, nb) * rows, rows)
        loads.append((
            pltpu.make_async_copy(rate.at[pl.ds(start, rows)], r_own.at[w], rl_sem.at[w]),
            pltpu.make_async_copy(mask.at[pl.ds(start, rows)], m_own.at[w], ml_sem.at[w]),
        ))
    for pair in loads:
        for cp in pair:
            cp.start()

    def device(r, b):
        return dict(device_id={"rep": r, "blk": b}, device_id_type=MESH_ID)

    def tell(*who):
        for r, b in who:
            pl.semaphore_signal(barrier, inc=1, **device(r, b))

    def encode(w):
        for cp in loads[w]:
            cp.wait()
        r_own[w] = jnp.where(m_own[w] != 0, r_own[w], jnp.inf)

    def send_factors():
        cps = [
            pltpu.make_async_remote_copy(ut_in, ut_land.at[me], us_sem, u_sem.at[me], **device(rep, lead)),
            pltpu.make_async_remote_copy(vt_in, vt_land.at[me], vs_sem, v_sem.at[me], **device(rep, lead)),
        ]
        for cp in cps:
            cp.start()
        return cps

    def send_block(w):
        cp = pltpu.make_async_remote_copy(
            r_own.at[w], r_all.at[w, me], s_sem.at[w], r_sem.at[w, me], **device(rep, lead)
        )
        cp.start()
        return cp

    def get_results():
        pltpu.make_async_copy(ut_out, ut_out, ou_sem).wait()
        pltpu.make_async_copy(vt_out, vt_out, ov_sem).wait()

    def finish(cps):
        for cp in cps:
            cp.wait_send()
        get_results()

    def part_rows(c):
        return pl.ds(c * hop_1.shape[2], hop_1.shape[2])

    def send_far(side):
        cps = send_factors()
        cps.append(send_block(0))
        for c in range(parts):
            cps.append(pltpu.make_async_remote_copy(
                r_own.at[late, part_rows(c)], hop_1.at[side, c], h1s_sem.at[c], h1_sem.at[side, c],
                **device(other, 2 * other),
            ))
            cps[-1].start()
        for w in range(1, late):
            encode(w)
        for w in range(1, late):
            cps.append(send_block(w))
        return cps

    @pl.when(me == far_0)
    def _():
        tell((rep, lead))
        encode(0)
        encode(late)
        pl.semaphore_wait(barrier, 2)
        finish(send_far(0))

    @pl.when(me == far_1)
    def _():
        tell((rep, lead), (rep, mate))
        encode(0)
        encode(late)
        pl.semaphore_wait(barrier, 3)
        cps = send_far(1)
        for c in range(parts):
            for side in range(2):
                pltpu.make_async_copy(hop_2.at[side, c], hop_2.at[side, c], h2_sem.at[side, c]).wait()
                home = lax.rem(2 * other + 2 + side, nb)
                cps.append(pltpu.make_async_remote_copy(
                    hop_2.at[side, c], r_all.at[late, home, part_rows(c)], h3s_sem.at[side, c], h3_sem.at[side, c],
                    **device(other, 2 * other + 1),
                ))
                cps[-1].start()
        finish(cps)

    @pl.when(me == mate)
    def _():
        tell((rep, lead), (other, lax.rem(2 * other + 2, nb)), (other, lax.rem(2 * other + 3, nb)))
        encode(0)
        encode(1)
        pl.semaphore_wait(barrier, 2)
        cps = send_factors()
        cps.append(send_block(0))
        for w in range(2, nb):
            encode(w)
        for w in range(1, nb):
            cps.append(send_block(w))
        for c in range(parts):
            for side in range(2):
                pltpu.make_async_copy(hop_1.at[side, c], hop_1.at[side, c], h1_sem.at[side, c]).wait()
                cps.append(pltpu.make_async_remote_copy(
                    hop_1.at[side, c], hop_2.at[side, c], h2s_sem.at[side, c], h2_sem.at[side, c],
                    **device(rep, far_1),
                ))
                cps[-1].start()
        finish(cps)

    @pl.when(me == lead)
    def _():
        tell((rep, mate), (rep, far_0), (rep, far_1), (other, lax.rem(2 * other + 3, nb)))
        ut_land[lead] = ut_in[...]
        vt_land[lead] = vt_in[...]
        for w in range(nb):
            for cp in loads[w]:
                cp.wait()
            m_all[w, lead] = m_own[w].astype(F32).astype(BF16)
            r_all[w, lead] = r_own[w]
        pl.semaphore_wait(barrier, nb - 1)

        for b in (mate, far_0, far_1):
            pltpu.make_async_copy(ut_land.at[b], ut_land.at[b], u_sem.at[b]).wait()
            pltpu.make_async_copy(vt_land.at[b], vt_land.at[b], v_sem.at[b]).wait()
        for i in range(nb):
            v32[i] = jnp.zeros(v32.shape[1:], F32)
            v32[i, :rank] = vt_land[i]
            vb[i] = v32[i].astype(BF16)
            ut = jnp.concatenate([ut_land[i], jnp.zeros((rows - rank, rows), F32)], axis=0)
            u32[i] = ut.T[:, :KPAD]
            ub[i] = ut.T[:, :KPAD].astype(BF16)
            utb[i] = ut[:KPAD].astype(BF16)

        def run(order, t0, w_of, j_of):
            prod, grads = {}, {}
            for kind, s, i in order:
                sub = s // STEPS
                j, w = j_of(sub, i), w_of(sub)
                if kind == "A":
                    prod[s, i] = [dot(ub[i], vb[j, :, h]) for h in halves]
                elif kind == "B":
                    errs = [
                        (a - r_all[w, j, :, h]).astype(BF16) * m_all[w, j, :, h]
                        for a, h in zip(prod.pop((s, i)), halves)
                    ]
                    gu = [dot_nt(err, vb[j, :, h]) for err, h in zip(errs, halves)]
                    grads[s, i] = gu, [dot(utb[i], err) for err in errs]
                else:
                    eta = lr[s % STEPS, t0 + sub] * base_eta
                    keep = 1.0 - eta * LAMBDA
                    gu, gv = grads.pop((s, i))
                    u_new = u32[i] * keep - eta * gu[0] - eta * gu[1]
                    u32[i] = u_new
                    u_bf = u_new.astype(BF16)
                    ub[i] = u_bf
                    utb[i] = u_bf.T
                    for g, h in zip(gv, halves):
                        v_new = v32[j, :, h] * keep - eta * g
                        v32[j, :, h] = v_new
                        vb[j, :, h] = v_new.astype(BF16)

        order_1 = make_order(nb, 1, 3000)
        order_n = make_order(nb, UNROLL, 0)

        def first_epoch(w, carry):
            pltpu.make_async_copy(r_all.at[w, mate], r_all.at[w, mate], r_sem.at[w, mate]).wait()

            @pl.when(w < late)
            def _():
                for j in (far_0, far_1):
                    pltpu.make_async_copy(r_all.at[w, j], r_all.at[w, j], r_sem.at[w, j]).wait()

            @pl.when(w == late)
            def _():
                for c in range(parts):
                    for side, j in enumerate((far_0, far_1)):
                        dst = r_all.at[late, j, part_rows(c)]
                        pltpu.make_async_copy(dst, dst, h3_sem.at[side, c]).wait()

            for j in (mate, far_0, far_1):
                coded = r_all[w, j]
                seen = coded < jnp.inf
                m_all[w, j] = jnp.where(seen, 1.0, 0.0).astype(BF16)
                r_all[w, j] = jnp.where(seen, coded, 0.0)
            run(order_1, w, lambda sub: w, lambda sub, i: lax.rem(i - w + nb, nb))
            return carry

        def later(n, carry):
            run(order_n, nb + n * UNROLL, lambda sub: sub % nb, lambda sub, i: (i - sub) % nb)
            return carry

        lax.fori_loop(0, nb, first_epoch, 0)
        lax.fori_loop(0, (subs - nb) // UNROLL, later, 0)

        for i in range(nb):
            ut = jnp.concatenate([u32[i], jnp.zeros((rows, rows - KPAD), F32)], axis=1).T
            ut_land[i] = ut[:rank]
            vt_land[i] = v32[i, :rank]
        cps = []
        for n, j in enumerate((mate, far_0, far_1)):
            to = device(rep, j)
            cps.append(pltpu.make_async_remote_copy(vt_land.at[j], vt_out, ovs_sem.at[n], ov_sem, **to))
            cps.append(pltpu.make_async_remote_copy(ut_land.at[j], ut_out, ous_sem.at[n], ou_sem, **to))
        cps.reverse()
        for cp in cps:
            cp.start()
        mine = [
            pltpu.make_async_copy(ut_land.at[lead], ut_out, ou_sem),
            pltpu.make_async_copy(vt_land.at[lead], vt_out, ov_sem),
        ]
        for cp in mine:
            cp.start()
        for cp in mine:
            cp.wait()
        for cp in cps:
            cp.wait_send()


def solution(mesh):
    nb = mesh.shape["blk"]

    def local_run(rate_loc, mask_loc, user_loc, item_loc, lr_scale):
        rows, rank = user_loc.shape
        cols = item_loc.shape[0]
        base_eta = math.sqrt(rank) / (4.0 * (cols + 2 * rank))
        vmem = pl.BlockSpec(memory_space=pltpu.VMEM)
        hbm = pl.BlockSpec(memory_space=pl.ANY)
        dma = pltpu.SemaphoreType.DMA
        ut, vt = pl.pallas_call(
            functools.partial(kernel, nb, rank, base_eta),
            out_shape=(jax.ShapeDtypeStruct((rank, rows), F32), jax.ShapeDtypeStruct((rank, cols), F32)),
            in_specs=[pl.BlockSpec(memory_space=pltpu.SMEM), hbm, hbm, vmem, vmem],
            out_specs=(hbm, hbm),
            scratch_shapes=[
                pltpu.VMEM((nb, nb, rows, cols), F32),
                pltpu.VMEM((nb, nb, rows, cols), BF16),
                pltpu.VMEM((nb, rows, cols), F32),
                pltpu.VMEM((nb, rows, cols), jnp.int32),
                pltpu.VMEM((2, 4, rows // 4, cols), F32),
                pltpu.VMEM((2, 4, rows // 4, cols), F32),
                pltpu.VMEM((nb, rank, rows), F32),
                pltpu.VMEM((nb, rank, cols), F32),
                pltpu.VMEM((nb, rows, KPAD), F32),
                pltpu.VMEM((nb, KPAD, cols), F32),
                pltpu.VMEM((nb, rows, KPAD), BF16),
                pltpu.VMEM((nb, KPAD, rows), BF16),
                pltpu.VMEM((nb, KPAD, cols), BF16),
                dma((nb,)), dma((nb,)),
                dma((nb, nb)), dma((nb,)), dma((nb,)), dma((nb,)), dma, dma,
                dma, dma, dma((nb - 1,)), dma((nb - 1,)),
                dma((2, 4)), dma((4,)), dma((2, 4)), dma((2, 4)), dma((2, 4)), dma((2, 4)),
            ],
            compiler_params=pltpu.CompilerParams(collective_id=0, has_side_effects=True),
            name="dsgd",
        )(lr_scale.T, rate_loc, mask_loc, user_loc.T, item_loc.T)
        return ut.T, vt.T

    spec_cols = P(None, ("rep", "blk"))
    spec_rows = P(("rep", "blk"), None)
    return jax.shard_map(
        local_run,
        mesh=mesh,
        in_specs=(spec_cols, spec_cols, spec_rows, spec_rows, P(None, None)),
        out_specs=(spec_rows, spec_rows),
        check_vma=False,
    )
```

```python
import functools
import math
import random

import jax
import jax.numpy as jnp
from jax import lax
from jax.experimental import pallas as pl
from jax.experimental.pallas import tpu as pltpu
from jax.sharding import PartitionSpec as P

LAMBDA = 0.05
STEPS = 4
KPAD = 64
UNROLL = 12
LEN_A, LEN_B, A_TO_B, B_TO_C, LEN_C = 64, 96, 226, 211, 35
F32 = jnp.float32
BF16 = jnp.bfloat16
MESH_ID = pl.DeviceIdType.MESH


def play(order, nb):
    now, start, done = 0, {}, {}
    for kind, s, i in order:
        if kind == 0:
            ready = 0
            if s > 0:
                before = [(s - 1, i)] + ([(s - 1, (i - 1) % nb)] if s % STEPS == 0 else [])
                if any(d not in done for d in before):
                    return None
                ready = max(done[d] for d in before)
            now = max(now, ready)
            start[kind, s, i] = now
            now += LEN_A
        else:
            if (0, s, i) not in start:
                return None
            now = max(now, start[0, s, i] + A_TO_B)
            start[kind, s, i] = now
            now += LEN_B
            done[s, i] = now + B_TO_C + LEN_C
    return now, start


def repeat(place, nb, subs):
    keys = [(t + u * 2 * STEPS * nb, kind, s + u * STEPS, i) for u in range(subs) for (kind, s, i), t in place.items()]
    return [k[1:] for k in sorted(keys)]


def find_places(nb, tries, seed):
    place = {}
    for n in range(STEPS * nb):
        s, i = n // nb, nb - 1 - n % nb
        place[0, s, i], place[1, s, i] = 2.0 * n, 2.0 * n + 3.0
    rnd = random.Random(seed)
    names = list(place)
    cur = best = place
    length = low = play(repeat(place, nb, 5), nb)[0]
    for it in range(tries):
        new = dict(cur)
        new[rnd.choice(names)] += rnd.choice((-4.5, -3.5, -2.5, -1.5, 1.5, 2.5, 3.5, 4.5)) + rnd.uniform(-0.2, 0.2)
        played = play(repeat(new, nb, 5), nb)
        if played is None:
            continue
        temp = 60 * (1 - it / tries) + 0.5
        if played[0] <= length or rnd.random() < math.exp((length - played[0]) / temp):
            cur, length = new, played[0]
            if length < low:
                best, low = new, length
    return best


def make_order(place, nb, subs):
    start = play(repeat(place, nb, subs), nb)[1]
    events = [(t, 1, "AB"[key[0]], *key[1:]) for key, t in start.items()]
    events += [(t + LEN_B + B_TO_C, 0, "C", *key[1:]) for key, t in start.items() if key[0] == 1]
    return [e[2:] for e in sorted(events)]


def dot(a, b):
    return jnp.dot(a, b, preferred_element_type=F32)


def dot_nt(a, b):
    return lax.dot_general(a, b, (((1,), (1,)), ((), ())), preferred_element_type=F32)


def kernel(nb, rank, base_eta, lr, rate, mask, ut_in, vt_in, ut_out, vt_out,
           r_all, m_all, r_own, m_own, hop_1, hop_2, ut_land, vt_land, u32, v32, ub, utb, vb,
           rl_sem, ml_sem, r_sem, s_sem, u_sem, v_sem, us_sem, vs_sem, ou_sem, ov_sem, ous_sem, ovs_sem,
           h1_sem, h1s_sem, h2_sem, h2s_sem, h3_sem, h3s_sem):
    me = lax.axis_index("blk")
    rep = lax.axis_index("rep")
    other = 1 - rep
    lead = 2 * rep + 1
    mate = 2 * rep
    far_0 = lax.rem(lead + 1, nb)
    far_1 = lax.rem(lead + 2, nb)
    late = nb - 2
    direct = [w for w in range(nb) if w != late]
    parts = hop_1.shape[1]
    rows, cols = r_all.shape[2:]
    subs = lr.shape[1]
    half = cols // 2
    halves = [slice(h * half, (h + 1) * half) for h in range(2)]
    barrier = pltpu.get_barrier_semaphore()

    loads = []
    for w in range(nb):
        start = pl.multiple_of(lax.rem(me + w, nb) * rows, rows)
        loads.append((
            pltpu.make_async_copy(rate.at[pl.ds(start, rows)], r_own.at[w], rl_sem.at[w]),
            pltpu.make_async_copy(mask.at[pl.ds(start, rows)], m_own.at[w], ml_sem.at[w]),
        ))
    for pair in loads:
        for cp in pair:
            cp.start()

    def device(r, b):
        return dict(device_id={"rep": r, "blk": b}, device_id_type=MESH_ID)

    def tell(*who):
        for r, b in who:
            pl.semaphore_signal(barrier, inc=1, **device(r, b))

    def encode(w):
        for cp in loads[w]:
            cp.wait()
        r_own[w] = jnp.where(m_own[w] != 0, r_own[w], jnp.inf)

    def send_factors():
        cps = [
            pltpu.make_async_remote_copy(ut_in, ut_land.at[me], us_sem, u_sem.at[me], **device(rep, lead)),
            pltpu.make_async_remote_copy(vt_in, vt_land.at[me], vs_sem, v_sem.at[me], **device(rep, lead)),
        ]
        for cp in cps:
            cp.start()
        return cps

    def send_block(w):
        cp = pltpu.make_async_remote_copy(
            r_own.at[w], r_all.at[w, me], s_sem.at[w], r_sem.at[w, me], **device(rep, lead)
        )
        cp.start()
        return cp

    def get_results():
        pltpu.make_async_copy(ut_out, ut_out, ou_sem).wait()
        pltpu.make_async_copy(vt_out, vt_out, ov_sem).wait()

    def finish(cps):
        for cp in cps:
            cp.wait_send()
        get_results()

    def part_rows(c):
        return pl.ds(c * hop_1.shape[2], hop_1.shape[2])

    def send_far(side):
        cps = send_factors()
        cps.append(send_block(0))
        for c in range(parts):
            cps.append(pltpu.make_async_remote_copy(
                r_own.at[late, part_rows(c)], hop_1.at[side, c], h1s_sem.at[c], h1_sem.at[side, c],
                **device(other, 2 * other),
            ))
            cps[-1].start()
        for w in direct[1:]:
            encode(w)
        for w in direct[1:]:
            cps.append(send_block(w))
        return cps

    @pl.when(me == far_0)
    def _():
        tell((rep, lead))
        encode(0)
        encode(late)
        pl.semaphore_wait(barrier, 2)
        finish(send_far(0))

    @pl.when(me == far_1)
    def _():
        tell((rep, lead), (rep, mate))
        encode(0)
        encode(late)
        pl.semaphore_wait(barrier, 3)
        cps = send_far(1)
        for c in range(parts):
            for side in range(2):
                pltpu.make_async_copy(hop_2.at[side, c], hop_2.at[side, c], h2_sem.at[side, c]).wait()
                home = lax.rem(2 * other + 2 + side, nb)
                cps.append(pltpu.make_async_remote_copy(
                    hop_2.at[side, c], r_all.at[late, home, part_rows(c)], h3s_sem.at[side, c], h3_sem.at[side, c],
                    **device(other, 2 * other + 1),
                ))
                cps[-1].start()
        finish(cps)

    @pl.when(me == mate)
    def _():
        tell((rep, lead), (other, lax.rem(2 * other + 2, nb)), (other, lax.rem(2 * other + 3, nb)))
        encode(0)
        encode(1)
        pl.semaphore_wait(barrier, 2)
        cps = send_factors()
        cps.append(send_block(0))
        for w in range(2, nb):
            encode(w)
        for w in range(1, nb):
            cps.append(send_block(w))
        for c in range(parts):
            for side in range(2):
                pltpu.make_async_copy(hop_1.at[side, c], hop_1.at[side, c], h1_sem.at[side, c]).wait()
                cps.append(pltpu.make_async_remote_copy(
                    hop_1.at[side, c], hop_2.at[side, c], h2s_sem.at[side, c], h2_sem.at[side, c],
                    **device(rep, far_1),
                ))
                cps[-1].start()
        finish(cps)

    @pl.when(me == lead)
    def _():
        tell((rep, mate), (rep, far_0), (rep, far_1), (other, lax.rem(2 * other + 3, nb)))
        ut_land[lead] = ut_in[...]
        vt_land[lead] = vt_in[...]
        for w in range(nb):
            for cp in loads[w]:
                cp.wait()
            m_all[w, lead] = m_own[w].astype(F32).astype(BF16)
            r_all[w, lead] = r_own[w]
        pl.semaphore_wait(barrier, nb - 1)

        for b in (mate, far_0, far_1):
            pltpu.make_async_copy(ut_land.at[b], ut_land.at[b], u_sem.at[b]).wait()
            pltpu.make_async_copy(vt_land.at[b], vt_land.at[b], v_sem.at[b]).wait()
        for i in range(nb):
            v32[i] = jnp.zeros(v32.shape[1:], F32)
            v32[i, :rank] = vt_land[i]
            vb[i] = v32[i].astype(BF16)
            ut = jnp.concatenate([ut_land[i], jnp.zeros((rows - rank, rows), F32)], axis=0)
            u32[i] = ut.T[:, :KPAD]
            ub[i] = ut.T[:, :KPAD].astype(BF16)
            utb[i] = ut[:KPAD].astype(BF16)

        def run(order, t0, w_of, j_of):
            prod, grads = {}, {}
            for kind, s, i in order:
                sub = s // STEPS
                j, w = j_of(sub, i), w_of(sub)
                if kind == "A":
                    prod[s, i] = [dot(ub[i], vb[j, :, h]) for h in halves]
                elif kind == "B":
                    errs = [
                        (a - r_all[w, j, :, h]).astype(BF16) * m_all[w, j, :, h]
                        for a, h in zip(prod.pop((s, i)), halves)
                    ]
                    gu = [dot_nt(err, vb[j, :, h]) for err, h in zip(errs, halves)]
                    grads[s, i] = gu, [dot(utb[i], err) for err in errs]
                else:
                    eta = lr[s % STEPS, t0 + sub] * base_eta
                    keep = 1.0 - eta * LAMBDA
                    gu, gv = grads.pop((s, i))
                    u_new = u32[i] * keep - eta * gu[0] - eta * gu[1]
                    u32[i] = u_new
                    u_bf = u_new.astype(BF16)
                    ub[i] = u_bf
                    utb[i] = u_bf.T
                    for g, h in zip(gv, halves):
                        v_new = v32[j, :, h] * keep - eta * g
                        v32[j, :, h] = v_new
                        vb[j, :, h] = v_new.astype(BF16)

        place = find_places(nb, 12000, 1)
        order_1 = make_order(place, nb, 1)
        order_n = make_order(place, nb, UNROLL)

        def first_epoch(w, carry):
            pltpu.make_async_copy(r_all.at[w, mate], r_all.at[w, mate], r_sem.at[w, mate]).wait()

            @pl.when(w != late)
            def _():
                for j in (far_0, far_1):
                    pltpu.make_async_copy(r_all.at[w, j], r_all.at[w, j], r_sem.at[w, j]).wait()

            @pl.when(w == late)
            def _():
                for c in range(parts):
                    for side, j in enumerate((far_0, far_1)):
                        dst = r_all.at[late, j, part_rows(c)]
                        pltpu.make_async_copy(dst, dst, h3_sem.at[side, c]).wait()

            for j in (mate, far_0, far_1):
                coded = r_all[w, j]
                seen = coded < jnp.inf
                m_all[w, j] = jnp.where(seen, 1.0, 0.0).astype(BF16)
                r_all[w, j] = jnp.where(seen, coded, 0.0)
            run(order_1, w, lambda sub: w, lambda sub, i: lax.rem(i - w + nb, nb))
            return carry

        def later(n, carry):
            run(order_n, nb + n * UNROLL, lambda sub: sub % nb, lambda sub, i: (i - sub) % nb)
            return carry

        lax.fori_loop(0, nb, first_epoch, 0)
        lax.fori_loop(0, (subs - nb) // UNROLL, later, 0)

        for i in range(nb):
            ut = jnp.concatenate([u32[i], jnp.zeros((rows, rows - KPAD), F32)], axis=1).T
            ut_land[i] = ut[:rank]
            vt_land[i] = v32[i, :rank]
        cps = []
        for n, j in enumerate((mate, far_0, far_1)):
            to = device(rep, j)
            cps.append(pltpu.make_async_remote_copy(vt_land.at[j], vt_out, ovs_sem.at[n], ov_sem, **to))
            cps.append(pltpu.make_async_remote_copy(ut_land.at[j], ut_out, ous_sem.at[n], ou_sem, **to))
        cps.reverse()
        for cp in cps:
            cp.start()
        mine = [
            pltpu.make_async_copy(ut_land.at[lead], ut_out, ou_sem),
            pltpu.make_async_copy(vt_land.at[lead], vt_out, ov_sem),
        ]
        for cp in mine:
            cp.start()
        for cp in mine:
            cp.wait()
        for cp in cps:
            cp.wait_send()


def solution(mesh):
    nb = mesh.shape["blk"]

    def local_run(rate_loc, mask_loc, user_loc, item_loc, lr_scale):
        rows, rank = user_loc.shape
        cols = item_loc.shape[0]
        base_eta = math.sqrt(rank) / (4.0 * (cols + 2 * rank))
        vmem = pl.BlockSpec(memory_space=pltpu.VMEM)
        hbm = pl.BlockSpec(memory_space=pl.ANY)
        dma = pltpu.SemaphoreType.DMA
        ut, vt = pl.pallas_call(
            functools.partial(kernel, nb, rank, base_eta),
            out_shape=(jax.ShapeDtypeStruct((rank, rows), F32), jax.ShapeDtypeStruct((rank, cols), F32)),
            in_specs=[pl.BlockSpec(memory_space=pltpu.SMEM), hbm, hbm, vmem, vmem],
            out_specs=(hbm, hbm),
            scratch_shapes=[
                pltpu.VMEM((nb, nb, rows, cols), F32),
                pltpu.VMEM((nb, nb, rows, cols), BF16),
                pltpu.VMEM((nb, rows, cols), F32),
                pltpu.VMEM((nb, rows, cols), jnp.int32),
                pltpu.VMEM((2, 4, rows // 4, cols), F32),
                pltpu.VMEM((2, 4, rows // 4, cols), F32),
                pltpu.VMEM((nb, rank, rows), F32),
                pltpu.VMEM((nb, rank, cols), F32),
                pltpu.VMEM((nb, rows, KPAD), F32),
                pltpu.VMEM((nb, KPAD, cols), F32),
                pltpu.VMEM((nb, rows, KPAD), BF16),
                pltpu.VMEM((nb, KPAD, rows), BF16),
                pltpu.VMEM((nb, KPAD, cols), BF16),
                dma((nb,)), dma((nb,)),
                dma((nb, nb)), dma((nb,)), dma((nb,)), dma((nb,)), dma, dma,
                dma, dma, dma((nb - 1,)), dma((nb - 1,)),
                dma((2, 4)), dma((4,)), dma((2, 4)), dma((2, 4)), dma((2, 4)), dma((2, 4)),
            ],
            compiler_params=pltpu.CompilerParams(collective_id=0, has_side_effects=True),
            name="dsgd",
        )(lr_scale.T, rate_loc, mask_loc, user_loc.T, item_loc.T)
        return ut.T, vt.T

    spec_cols = P(None, ("rep", "blk"))
    spec_rows = P(("rep", "blk"), None)
    return jax.shard_map(
        local_run,
        mesh=mesh,
        in_specs=(spec_cols, spec_cols, spec_rows, spec_rows, P(None, None)),
        out_specs=(spec_rows, spec_rows),
        check_vma=False,
    )
```

```python
import functools
import math
import random

import jax
import jax.numpy as jnp
from jax import lax
from jax.experimental import pallas as pl
from jax.experimental.pallas import tpu as pltpu
from jax.sharding import PartitionSpec as P

LAMBDA = 0.05
STEPS = 4
KPAD = 64
UNROLL = 12
LEN_A, LEN_B, A_TO_B, B_TO_C, LEN_C = 64, 96, 226, 211, 35
F32 = jnp.float32
BF16 = jnp.bfloat16
MESH_ID = pl.DeviceIdType.MESH


def play(order, nb):
    now, start, done = 0, {}, {}
    for kind, s, i in order:
        if kind == 0:
            ready = 0
            if s > 0:
                before = [(s - 1, i)] + ([(s - 1, (i - 1) % nb)] if s % STEPS == 0 else [])
                if any(d not in done for d in before):
                    return None
                ready = max(done[d] for d in before)
            now = max(now, ready)
            start[kind, s, i] = now
            now += LEN_A
        else:
            if (0, s, i) not in start:
                return None
            now = max(now, start[0, s, i] + A_TO_B)
            start[kind, s, i] = now
            now += LEN_B
            done[s, i] = now + B_TO_C + LEN_C
    return now, start


def repeat(place, nb, subs):
    keys = [(t + u * 2 * STEPS * nb, kind, s + u * STEPS, i) for u in range(subs) for (kind, s, i), t in place.items()]
    return [k[1:] for k in sorted(keys)]


def find_places(nb, tries, seed):
    place = {}
    for n in range(STEPS * nb):
        s, i = n // nb, nb - 1 - n % nb
        place[0, s, i], place[1, s, i] = 2.0 * n, 2.0 * n + 3.0
    rnd = random.Random(seed)
    names = list(place)
    cur = best = place
    length = low = play(repeat(place, nb, 5), nb)[0]
    for it in range(tries):
        new = dict(cur)
        new[rnd.choice(names)] += rnd.choice((-4.5, -3.5, -2.5, -1.5, 1.5, 2.5, 3.5, 4.5)) + rnd.uniform(-0.2, 0.2)
        played = play(repeat(new, nb, 5), nb)
        if played is None:
            continue
        temp = 60 * (1 - it / tries) + 0.5
        if played[0] <= length or rnd.random() < math.exp((length - played[0]) / temp):
            cur, length = new, played[0]
            if length < low:
                best, low = new, length
    return best


def make_order(place, nb, subs):
    start = play(repeat(place, nb, subs), nb)[1]
    events = [(t, 1, "AB"[key[0]], *key[1:]) for key, t in start.items()]
    events += [(t + LEN_B + B_TO_C, 0, "C", *key[1:]) for key, t in start.items() if key[0] == 1]
    return [e[2:] for e in sorted(events)]


def dot(a, b):
    return jnp.dot(a, b, preferred_element_type=F32)


def dot_nt(a, b):
    return lax.dot_general(a, b, (((1,), (1,)), ((), ())), preferred_element_type=F32)


def kernel(nb, rank, base_eta, lr, rate, mask, ut_in, vt_in, ut_out, vt_out,
           r_all, m_all, r_own, m_own, hop_1, hop_2, ut_land, vt_land, u32, v32, ub, utb, vb,
           rl_sem, ml_sem, r_sem, s_sem, u_sem, v_sem, us_sem, vs_sem, ou_sem, ov_sem, ous_sem, ovs_sem,
           h1_sem, h1s_sem, h2_sem, h2s_sem, h3_sem, h3s_sem):
    me = lax.axis_index("blk")
    rep = lax.axis_index("rep")
    other = 1 - rep
    lead = 2 * rep + 1
    mate = 2 * rep
    far_0 = lax.rem(lead + 1, nb)
    far_1 = lax.rem(lead + 2, nb)
    late = nb - 2
    direct = [w for w in range(nb) if w != late]
    parts = hop_1.shape[1]
    rows, cols = r_all.shape[2:]
    subs = lr.shape[1]
    half = cols // 2
    halves = [slice(h * half, (h + 1) * half) for h in range(2)]
    barrier = pltpu.get_barrier_semaphore()

    loads = []
    for w in range(nb):
        start = pl.multiple_of(lax.rem(me + w, nb) * rows, rows)
        loads.append((
            pltpu.make_async_copy(rate.at[pl.ds(start, rows)], r_own.at[w], rl_sem.at[w]),
            pltpu.make_async_copy(mask.at[pl.ds(start, rows)], m_own.at[w], ml_sem.at[w]),
        ))
    for pair in loads:
        for cp in pair:
            cp.start()

    def device(r, b):
        return dict(device_id={"rep": r, "blk": b}, device_id_type=MESH_ID)

    def tell(*who):
        for r, b in who:
            pl.semaphore_signal(barrier, inc=1, **device(r, b))

    def encode(w):
        for cp in loads[w]:
            cp.wait()
        r_own[w] = jnp.where(m_own[w] != 0, r_own[w], jnp.inf)

    def send_factors():
        cps = [
            pltpu.make_async_remote_copy(ut_in, ut_land.at[me], us_sem, u_sem.at[me], **device(rep, lead)),
            pltpu.make_async_remote_copy(vt_in, vt_land.at[me], vs_sem, v_sem.at[me], **device(rep, lead)),
        ]
        for cp in cps:
            cp.start()
        return cps

    def send_block(w):
        cp = pltpu.make_async_remote_copy(
            r_own.at[w], r_all.at[w, me], s_sem.at[w], r_sem.at[w, me], **device(rep, lead)
        )
        cp.start()
        return cp

    def get_results():
        pltpu.make_async_copy(ut_out, ut_out, ou_sem).wait()
        pltpu.make_async_copy(vt_out, vt_out, ov_sem).wait()

    def finish(cps):
        for cp in cps:
            cp.wait_send()
        get_results()

    def part_rows(c):
        return pl.ds(c * hop_1.shape[2], hop_1.shape[2])

    def send_far(side):
        cps = send_factors()
        cps.append(send_block(0))
        for c in range(parts):
            cps.append(pltpu.make_async_remote_copy(
                r_own.at[late, part_rows(c)], hop_1.at[side, c], h1s_sem.at[c], h1_sem.at[side, c],
                **device(other, 2 * other),
            ))
            cps[-1].start()
        for w in direct[1:]:
            encode(w)
        for w in direct[1:]:
            cps.append(send_block(w))
        return cps

    @pl.when(me == far_0)
    def _():
        tell((rep, lead))
        encode(0)
        encode(late)
        pl.semaphore_wait(barrier, 2)
        finish(send_far(0))

    @pl.when(me == far_1)
    def _():
        tell((rep, lead), (rep, mate))
        encode(0)
        encode(late)
        pl.semaphore_wait(barrier, 3)
        cps = send_far(1)
        for c in range(parts):
            for side in range(2):
                pltpu.make_async_copy(hop_2.at[side, c], hop_2.at[side, c], h2_sem.at[side, c]).wait()
                home = lax.rem(2 * other + 2 + side, nb)
                cps.append(pltpu.make_async_remote_copy(
                    hop_2.at[side, c], r_all.at[late, home, part_rows(c)], h3s_sem.at[side, c], h3_sem.at[side, c],
                    **device(other, 2 * other + 1),
                ))
                cps[-1].start()
        finish(cps)

    @pl.when(me == mate)
    def _():
        tell((rep, lead), (other, lax.rem(2 * other + 2, nb)), (other, lax.rem(2 * other + 3, nb)))
        encode(0)
        encode(1)
        pl.semaphore_wait(barrier, 2)
        cps = send_factors()
        cps.append(send_block(0))
        for w in range(2, nb):
            encode(w)
        for w in range(1, nb):
            cps.append(send_block(w))
        for c in range(parts):
            for side in range(2):
                pltpu.make_async_copy(hop_1.at[side, c], hop_1.at[side, c], h1_sem.at[side, c]).wait()
                cps.append(pltpu.make_async_remote_copy(
                    hop_1.at[side, c], hop_2.at[side, c], h2s_sem.at[side, c], h2_sem.at[side, c],
                    **device(rep, far_1),
                ))
                cps[-1].start()
        finish(cps)

    @pl.when(me == lead)
    def _():
        tell((rep, mate), (rep, far_0), (rep, far_1), (other, lax.rem(2 * other + 3, nb)))
        ut_land[lead] = ut_in[...]
        vt_land[lead] = vt_in[...]
        for w in range(nb):
            for cp in loads[w]:
                cp.wait()
            m_all[w, lead] = m_own[w].astype(F32).astype(BF16)
            r_all[w, lead] = r_own[w]
        pl.semaphore_wait(barrier, nb - 1)

        for b in (mate, far_0, far_1):
            pltpu.make_async_copy(ut_land.at[b], ut_land.at[b], u_sem.at[b]).wait()
            pltpu.make_async_copy(vt_land.at[b], vt_land.at[b], v_sem.at[b]).wait()
        for i in range(nb):
            v32[i] = jnp.zeros(v32.shape[1:], F32)
            v32[i, :rank] = vt_land[i]
            vb[i] = v32[i].astype(BF16)
            ut = jnp.concatenate([ut_land[i], jnp.zeros((rows - rank, rows), F32)], axis=0)
            u32[i] = ut.T[:, :KPAD]
            ub[i] = ut.T[:, :KPAD].astype(BF16)
            utb[i] = ut[:KPAD].astype(BF16)

        def run(order, t0, w_of, j_of):
            prod, grads = {}, {}
            for kind, s, i in order:
                sub = s // STEPS
                j, w = j_of(sub, i), w_of(sub)
                if kind == "A":
                    prod[s, i] = [dot(ub[i], vb[j, :, h]) for h in halves]
                elif kind == "B":
                    errs = [
                        (a - r_all[w, j, :, h]).astype(BF16) * m_all[w, j, :, h]
                        for a, h in zip(prod.pop((s, i)), halves)
                    ]
                    gu = [dot_nt(err, vb[j, :, h]) for err, h in zip(errs, halves)]
                    grads[s, i] = gu, [dot(utb[i], err) for err in errs]
                else:
                    eta = lr[s % STEPS, t0 + sub] * base_eta
                    keep = 1.0 - eta * LAMBDA
                    gu, gv = grads.pop((s, i))
                    u_new = u32[i] * keep - eta * gu[0] - eta * gu[1]
                    u32[i] = u_new
                    u_bf = u_new.astype(BF16)
                    ub[i] = u_bf
                    utb[i] = u_bf.T
                    for g, h in zip(gv, halves):
                        v_new = v32[j, :, h] * keep - eta * g
                        v32[j, :, h] = v_new
                        vb[j, :, h] = v_new.astype(BF16)

        place = find_places(nb, 12000, 1)
        order_1 = make_order(place, nb, 1)
        order_n = make_order(place, nb, UNROLL)

        def first_epoch(w, carry):
            pltpu.make_async_copy(r_all.at[w, mate], r_all.at[w, mate], r_sem.at[w, mate]).wait()

            @pl.when(w != late)
            def _():
                for j in (far_0, far_1):
                    pltpu.make_async_copy(r_all.at[w, j], r_all.at[w, j], r_sem.at[w, j]).wait()

            @pl.when(w == late)
            def _():
                for c in range(parts):
                    for side, j in enumerate((far_0, far_1)):
                        dst = r_all.at[late, j, part_rows(c)]
                        pltpu.make_async_copy(dst, dst, h3_sem.at[side, c]).wait()

            for j in (mate, far_0, far_1):
                coded = r_all[w, j]
                seen = coded < jnp.inf
                m_all[w, j] = jnp.where(seen, 1.0, 0.0).astype(BF16)
                r_all[w, j] = jnp.where(seen, coded, 0.0)
            run(order_1, w, lambda sub: w, lambda sub, i: lax.rem(i - w + nb, nb))
            return carry

        def later(n, carry):
            run(order_n, nb + n * UNROLL, lambda sub: sub % nb, lambda sub, i: (i - sub) % nb)
            return carry

        lax.fori_loop(0, nb, first_epoch, 0)
        lax.fori_loop(0, (subs - nb) // UNROLL, later, 0)

        for i in range(nb):
            ut = jnp.concatenate([u32[i], jnp.zeros((rows, rows - KPAD), F32)], axis=1).T
            ut_land[i] = ut[:rank]
            vt_land[i] = v32[i, :rank]
        cps = []
        for n, j in enumerate((mate, far_0, far_1)):
            to = device(rep, j)
            cps.append(pltpu.make_async_remote_copy(vt_land.at[j], vt_out, ovs_sem.at[n], ov_sem, **to))
            cps.append(pltpu.make_async_remote_copy(ut_land.at[j], ut_out, ous_sem.at[n], ou_sem, **to))
        cps.reverse()
        for cp in cps:
            cp.start()
        mine = [
            pltpu.make_async_copy(ut_land.at[lead], ut_out, ou_sem),
            pltpu.make_async_copy(vt_land.at[lead], vt_out, ov_sem),
        ]
        for cp in mine:
            cp.start()
        for cp in mine:
            cp.wait()
        for cp in cps:
            cp.wait_send()


def solution(mesh):
    nb = mesh.shape["blk"]

    def local_run(rate_loc, mask_loc, user_loc, item_loc, lr_scale):
        rows, rank = user_loc.shape
        cols = item_loc.shape[0]
        base_eta = math.sqrt(rank) / (4.0 * (cols + 2 * rank))
        vmem = pl.BlockSpec(memory_space=pltpu.VMEM)
        hbm = pl.BlockSpec(memory_space=pltpu.HBM)
        anywhere = pl.BlockSpec(memory_space=pl.ANY)
        dma = pltpu.SemaphoreType.DMA
        ut, vt = pl.pallas_call(
            functools.partial(kernel, nb, rank, base_eta),
            out_shape=(jax.ShapeDtypeStruct((rank, rows), F32), jax.ShapeDtypeStruct((rank, cols), F32)),
            in_specs=[pl.BlockSpec(memory_space=pltpu.SMEM), hbm, hbm, vmem, vmem],
            out_specs=(anywhere, anywhere),
            scratch_shapes=[
                pltpu.VMEM((nb, nb, rows, cols), F32),
                pltpu.VMEM((nb, nb, rows, cols), BF16),
                pltpu.VMEM((nb, rows, cols), F32),
                pltpu.VMEM((nb, rows, cols), jnp.int32),
                pltpu.VMEM((2, 4, rows // 4, cols), F32),
                pltpu.VMEM((2, 4, rows // 4, cols), F32),
                pltpu.VMEM((nb, rank, rows), F32),
                pltpu.VMEM((nb, rank, cols), F32),
                pltpu.VMEM((nb, rows, KPAD), F32),
                pltpu.VMEM((nb, KPAD, cols), F32),
                pltpu.VMEM((nb, rows, KPAD), BF16),
                pltpu.VMEM((nb, KPAD, rows), BF16),
                pltpu.VMEM((nb, KPAD, cols), BF16),
                dma((nb,)), dma((nb,)),
                dma((nb, nb)), dma((nb,)), dma((nb,)), dma((nb,)), dma, dma,
                dma, dma, dma((nb - 1,)), dma((nb - 1,)),
                dma((2, 4)), dma((4,)), dma((2, 4)), dma((2, 4)), dma((2, 4)), dma((2, 4)),
            ],
            compiler_params=pltpu.CompilerParams(collective_id=0, has_side_effects=True, vmem_limit_bytes=53 * 2**20),
            name="dsgd",
        )(lr_scale.T, rate_loc, mask_loc, user_loc.T, item_loc.T)
        return ut.T, vt.T

    spec_cols = P(None, ("rep", "blk"))
    spec_rows = P(("rep", "blk"), None)
    return jax.shard_map(
        local_run,
        mesh=mesh,
        in_specs=(spec_cols, spec_cols, spec_rows, spec_rows, P(None, None)),
        out_specs=(spec_rows, spec_rows),
        check_vma=False,
    )
```

```python
import functools
import math
import random

import jax
import jax.numpy as jnp
from jax import lax
from jax.experimental import pallas as pl
from jax.experimental.pallas import tpu as pltpu
from jax.sharding import PartitionSpec as P

LAMBDA = 0.05
STEPS = 4
KPAD = 64
UNROLL = 12
LEN_A, LEN_B, A_TO_B, B_TO_C, LEN_C = 64, 96, 226, 211, 35
F32 = jnp.float32
BF16 = jnp.bfloat16
MESH_ID = pl.DeviceIdType.MESH


def play(order, nb):
    now, start, done = 0, {}, {}
    for kind, s, i in order:
        if kind == 0:
            ready = 0
            if s > 0:
                before = [(s - 1, i)] + ([(s - 1, (i - 1) % nb)] if s % STEPS == 0 else [])
                if any(d not in done for d in before):
                    return None
                ready = max(done[d] for d in before)
            now = max(now, ready)
            start[kind, s, i] = now
            now += LEN_A
        else:
            if (0, s, i) not in start:
                return None
            now = max(now, start[0, s, i] + A_TO_B)
            start[kind, s, i] = now
            now += LEN_B
            done[s, i] = now + B_TO_C + LEN_C
    return now, start


def repeat(place, nb, subs):
    keys = [(t + u * 2 * STEPS * nb, kind, s + u * STEPS, i) for u in range(subs) for (kind, s, i), t in place.items()]
    return [k[1:] for k in sorted(keys)]


def find_places(nb, tries, seed):
    place = {}
    for n in range(STEPS * nb):
        s, i = n // nb, nb - 1 - n % nb
        place[0, s, i], place[1, s, i] = 2.0 * n, 2.0 * n + 3.0
    rnd = random.Random(seed)
    names = list(place)
    cur = best = place
    length = low = play(repeat(place, nb, 5), nb)[0]
    for it in range(tries):
        new = dict(cur)
        new[rnd.choice(names)] += rnd.choice((-4.5, -3.5, -2.5, -1.5, 1.5, 2.5, 3.5, 4.5)) + rnd.uniform(-0.2, 0.2)
        played = play(repeat(new, nb, 5), nb)
        if played is None:
            continue
        temp = 60 * (1 - it / tries) + 0.5
        if played[0] <= length or rnd.random() < math.exp((length - played[0]) / temp):
            cur, length = new, played[0]
            if length < low:
                best, low = new, length
    return best


def make_order(place, nb, subs):
    start = play(repeat(place, nb, subs), nb)[1]
    events = [(t, 1, "AB"[key[0]], *key[1:]) for key, t in start.items()]
    events += [(t + LEN_B + B_TO_C, 0, "C", *key[1:]) for key, t in start.items() if key[0] == 1]
    return [e[2:] for e in sorted(events)]


def dot(a, b):
    return jnp.dot(a, b, preferred_element_type=F32)


def dot_nt(a, b):
    return lax.dot_general(a, b, (((1,), (1,)), ((), ())), preferred_element_type=F32)


def kernel(nb, rank, base_eta, lr_in, rate, mask, ut_in, vt_in, ut_out, vt_out,
           r_all, m_all, r_own, m_own, hop_1, hop_2, ut_land, vt_land, u32, v32, ub, utb, vb,
           rl_sem, ml_sem, r_sem, s_sem, u_sem, v_sem, us_sem, vs_sem, ou_sem, ov_sem, ous_sem, ovs_sem,
           lr, lr_sem, h1_sem, h1s_sem, h2_sem, h2s_sem, h3_sem, h3s_sem):
    me = lax.axis_index("blk")
    rep = lax.axis_index("rep")
    other = 1 - rep
    lead = 2 * rep + 1
    mate = 2 * rep
    far_0 = lax.rem(lead + 1, nb)
    far_1 = lax.rem(lead + 2, nb)
    late = nb - 2
    direct = [w for w in range(nb) if w != late]
    parts = hop_1.shape[1]
    rows, cols = r_all.shape[2:]
    subs = lr.shape[1]
    half = cols // 2
    halves = [slice(h * half, (h + 1) * half) for h in range(2)]
    barrier = pltpu.get_barrier_semaphore()

    loads = []
    for w in range(nb):
        start = pl.multiple_of(lax.rem(me + w, nb) * rows, rows)
        loads.append((
            pltpu.make_async_copy(rate.at[pl.ds(start, rows)], r_own.at[w], rl_sem.at[w]),
            pltpu.make_async_copy(mask.at[pl.ds(start, rows)], m_own.at[w], ml_sem.at[w]),
        ))
    for pair in loads:
        for cp in pair:
            cp.start()

    def device(r, b):
        return dict(device_id={"rep": r, "blk": b}, device_id_type=MESH_ID)

    def tell(*who):
        for r, b in who:
            pl.semaphore_signal(barrier, inc=1, **device(r, b))

    def encode(w):
        for cp in loads[w]:
            cp.wait()
        r_own[w] = jnp.where(m_own[w] != 0, r_own[w], jnp.inf)

    def send_factors():
        cps = [
            pltpu.make_async_remote_copy(ut_in, ut_land.at[me], us_sem, u_sem.at[me], **device(rep, lead)),
            pltpu.make_async_remote_copy(vt_in, vt_land.at[me], vs_sem, v_sem.at[me], **device(rep, lead)),
        ]
        for cp in cps:
            cp.start()
        return cps

    def send_block(w):
        cp = pltpu.make_async_remote_copy(
            r_own.at[w], r_all.at[w, me], s_sem.at[w], r_sem.at[w, me], **device(rep, lead)
        )
        cp.start()
        return cp

    def get_results():
        pltpu.make_async_copy(ut_out, ut_out, ou_sem).wait()
        pltpu.make_async_copy(vt_out, vt_out, ov_sem).wait()

    def finish(cps):
        for cp in cps:
            cp.wait_send()
        get_results()

    def part_rows(c):
        return pl.ds(c * hop_1.shape[2], hop_1.shape[2])

    def send_far(side):
        cps = send_factors()
        cps.append(send_block(0))
        for c in range(parts):
            cps.append(pltpu.make_async_remote_copy(
                r_own.at[late, part_rows(c)], hop_1.at[side, c], h1s_sem.at[c], h1_sem.at[side, c],
                **device(other, 2 * other),
            ))
            cps[-1].start()
        for w in direct[1:]:
            encode(w)
        for w in direct[1:]:
            cps.append(send_block(w))
        return cps

    @pl.when(me == far_0)
    def _():
        tell((rep, lead))
        encode(0)
        encode(late)
        pl.semaphore_wait(barrier, 2)
        finish(send_far(0))

    @pl.when(me == far_1)
    def _():
        tell((rep, lead), (rep, mate))
        encode(0)
        encode(late)
        pl.semaphore_wait(barrier, 3)
        cps = send_far(1)
        for c in range(parts):
            for side in range(2):
                pltpu.make_async_copy(hop_2.at[side, c], hop_2.at[side, c], h2_sem.at[side, c]).wait()
                home = lax.rem(2 * other + 2 + side, nb)
                cps.append(pltpu.make_async_remote_copy(
                    hop_2.at[side, c], r_all.at[late, home, part_rows(c)], h3s_sem.at[side, c], h3_sem.at[side, c],
                    **device(other, 2 * other + 1),
                ))
                cps[-1].start()
        finish(cps)

    @pl.when(me == mate)
    def _():
        tell((rep, lead), (other, lax.rem(2 * other + 2, nb)), (other, lax.rem(2 * other + 3, nb)))
        encode(0)
        encode(1)
        pl.semaphore_wait(barrier, 2)
        cps = send_factors()
        cps.append(send_block(0))
        for w in range(2, nb):
            encode(w)
        for w in range(1, nb):
            cps.append(send_block(w))
        for c in range(parts):
            for side in range(2):
                pltpu.make_async_copy(hop_1.at[side, c], hop_1.at[side, c], h1_sem.at[side, c]).wait()
                cps.append(pltpu.make_async_remote_copy(
                    hop_1.at[side, c], hop_2.at[side, c], h2s_sem.at[side, c], h2_sem.at[side, c],
                    **device(rep, far_1),
                ))
                cps[-1].start()
        finish(cps)

    @pl.when(me == lead)
    def _():
        tell((rep, mate), (rep, far_0), (rep, far_1), (other, lax.rem(2 * other + 3, nb)))
        own = [
            pltpu.make_async_copy(ut_in, ut_land.at[lead], us_sem),
            pltpu.make_async_copy(vt_in, vt_land.at[lead], vs_sem),
            pltpu.make_async_copy(lr_in, lr, lr_sem),
        ]
        for cp in own:
            cp.start()
        for w in range(nb):
            for cp in loads[w]:
                cp.wait()
            m_all[w, lead] = m_own[w].astype(F32).astype(BF16)
            r_all[w, lead] = r_own[w]
        for cp in own:
            cp.wait()
        pl.semaphore_wait(barrier, nb - 1)

        for b in (mate, far_0, far_1):
            pltpu.make_async_copy(ut_land.at[b], ut_land.at[b], u_sem.at[b]).wait()
            pltpu.make_async_copy(vt_land.at[b], vt_land.at[b], v_sem.at[b]).wait()
        for i in range(nb):
            v32[i] = jnp.zeros(v32.shape[1:], F32)
            v32[i, :rank] = vt_land[i]
            vb[i] = v32[i].astype(BF16)
            ut = jnp.concatenate([ut_land[i], jnp.zeros((rows - rank, rows), F32)], axis=0)
            u32[i] = ut.T[:, :KPAD]
            ub[i] = ut.T[:, :KPAD].astype(BF16)
            utb[i] = ut[:KPAD].astype(BF16)

        def run(order, t0, w_of, j_of):
            prod, grads = {}, {}
            for kind, s, i in order:
                sub = s // STEPS
                j, w = j_of(sub, i), w_of(sub)
                if kind == "A":
                    prod[s, i] = [dot(ub[i], vb[j, :, h]) for h in halves]
                elif kind == "B":
                    errs = [
                        (a - r_all[w, j, :, h]).astype(BF16) * m_all[w, j, :, h]
                        for a, h in zip(prod.pop((s, i)), halves)
                    ]
                    gu = [dot_nt(err, vb[j, :, h]) for err, h in zip(errs, halves)]
                    grads[s, i] = gu, [dot(utb[i], err) for err in errs]
                else:
                    eta = lr[s % STEPS, t0 + sub] * base_eta
                    keep = 1.0 - eta * LAMBDA
                    gu, gv = grads.pop((s, i))
                    u_new = u32[i] * keep - eta * gu[0] - eta * gu[1]
                    u32[i] = u_new
                    u_bf = u_new.astype(BF16)
                    ub[i] = u_bf
                    utb[i] = u_bf.T
                    for g, h in zip(gv, halves):
                        v_new = v32[j, :, h] * keep - eta * g
                        v32[j, :, h] = v_new
                        vb[j, :, h] = v_new.astype(BF16)

        place = find_places(nb, 12000, 1)
        order_1 = make_order(place, nb, 1)
        order_n = make_order(place, nb, UNROLL)

        def first_epoch(w, carry):
            pltpu.make_async_copy(r_all.at[w, mate], r_all.at[w, mate], r_sem.at[w, mate]).wait()

            @pl.when(w != late)
            def _():
                for j in (far_0, far_1):
                    pltpu.make_async_copy(r_all.at[w, j], r_all.at[w, j], r_sem.at[w, j]).wait()

            @pl.when(w == late)
            def _():
                for c in range(parts):
                    for side, j in enumerate((far_0, far_1)):
                        dst = r_all.at[late, j, part_rows(c)]
                        pltpu.make_async_copy(dst, dst, h3_sem.at[side, c]).wait()

            for j in (mate, far_0, far_1):
                coded = r_all[w, j]
                seen = coded < jnp.inf
                m_all[w, j] = jnp.where(seen, 1.0, 0.0).astype(BF16)
                r_all[w, j] = jnp.where(seen, coded, 0.0)
            run(order_1, w, lambda sub: w, lambda sub, i: lax.rem(i - w + nb, nb))
            return carry

        def later(n, carry):
            run(order_n, nb + n * UNROLL, lambda sub: sub % nb, lambda sub, i: (i - sub) % nb)
            return carry

        lax.fori_loop(0, nb, first_epoch, 0)
        lax.fori_loop(0, (subs - nb) // UNROLL, later, 0)

        def stage(j):
            vt_land[j] = v32[j, :rank]
            ut_land[j] = jnp.concatenate([u32[j], jnp.zeros((rows, rows - KPAD), F32)], axis=1).T[:rank]

        def send_home(n, j):
            for src, dst, s_out, s_in in ((vt_land, vt_out, ovs_sem, ov_sem), (ut_land, ut_out, ous_sem, ou_sem)):
                cps.append(pltpu.make_async_remote_copy(src.at[j], dst, s_out.at[n], s_in, **device(rep, j)))
                cps[-1].start()

        cps = []
        stage(far_0)
        stage(far_1)
        send_home(0, far_0)
        send_home(1, far_1)
        stage(mate)
        vt_out[...] = v32[lead, :rank]
        send_home(2, mate)
        ut_out[...] = jnp.concatenate([u32[lead], jnp.zeros((rows, rows - KPAD), F32)], axis=1).T[:rank]
        for cp in cps:
            cp.wait_send()


def solution(mesh):
    nb = mesh.shape["blk"]

    def local_run(rate_loc, mask_loc, user_loc, item_loc, lr_scale):
        rows, rank = user_loc.shape
        cols = item_loc.shape[0]
        subs = lr_scale.shape[0]
        base_eta = math.sqrt(rank) / (4.0 * (cols + 2 * rank))
        anywhere = pl.BlockSpec(memory_space=pl.ANY)
        dma = pltpu.SemaphoreType.DMA
        ut, vt = pl.pallas_call(
            functools.partial(kernel, nb, rank, base_eta),
            out_shape=(pltpu.VMEM((rank, rows), F32), pltpu.VMEM((rank, cols), F32)),
            in_specs=[anywhere] * 5,
            out_specs=(pl.BlockSpec(memory_space=pltpu.VMEM),) * 2,
            scratch_shapes=[
                pltpu.VMEM((nb, nb, rows, cols), F32),
                pltpu.VMEM((nb, nb, rows, cols), BF16),
                pltpu.VMEM((nb, rows, cols), F32),
                pltpu.VMEM((nb, rows, cols), jnp.int32),
                pltpu.VMEM((2, 4, rows // 4, cols), F32),
                pltpu.VMEM((2, 4, rows // 4, cols), F32),
                pltpu.VMEM((nb, rank, rows), F32),
                pltpu.VMEM((nb, rank, cols), F32),
                pltpu.VMEM((nb, rows, KPAD), F32),
                pltpu.VMEM((nb, KPAD, cols), F32),
                pltpu.VMEM((nb, rows, KPAD), BF16),
                pltpu.VMEM((nb, KPAD, rows), BF16),
                pltpu.VMEM((nb, KPAD, cols), BF16),
                dma((nb,)), dma((nb,)),
                dma((nb, nb)), dma((nb,)), dma((nb,)), dma((nb,)), dma, dma,
                dma, dma, dma((nb - 1,)), dma((nb - 1,)),
                pltpu.SMEM((STEPS, subs), F32), dma,
                dma((2, 4)), dma((4,)), dma((2, 4)), dma((2, 4)), dma((2, 4)), dma((2, 4)),
            ],
            compiler_params=pltpu.CompilerParams(collective_id=0, has_side_effects=True),
            name="dsgd",
        )(lr_scale.T, rate_loc, mask_loc, user_loc.T, item_loc.T)
        return ut.T, vt.T

    spec_cols = P(None, ("rep", "blk"))
    spec_rows = P(("rep", "blk"), None)
    return jax.shard_map(
        local_run,
        mesh=mesh,
        in_specs=(spec_cols, spec_cols, spec_rows, spec_rows, P(None, None)),
        out_specs=(spec_rows, spec_rows),
        check_vma=False,
    )
```

```python
import functools
import math
import random

import jax
import jax.numpy as jnp
from jax import lax
from jax.experimental import pallas as pl
from jax.experimental.pallas import tpu as pltpu
from jax.sharding import PartitionSpec as P

LAMBDA = 0.05
STEPS = 4
KPAD = 64
UNROLL = 12
LEN_A, LEN_B, A_TO_B, B_TO_C, LEN_C = 64, 96, 226, 211, 35
F32 = jnp.float32
BF16 = jnp.bfloat16
MESH_ID = pl.DeviceIdType.MESH


def play(order, nb):
    now, start, done = 0, {}, {}
    for kind, s, i in order:
        if kind == 0:
            ready = 0
            if s > 0:
                before = [(s - 1, i)] + ([(s - 1, (i - 1) % nb)] if s % STEPS == 0 else [])
                if any(d not in done for d in before):
                    return None
                ready = max(done[d] for d in before)
            now = max(now, ready)
            start[kind, s, i] = now
            now += LEN_A
        else:
            if (0, s, i) not in start:
                return None
            now = max(now, start[0, s, i] + A_TO_B)
            start[kind, s, i] = now
            now += LEN_B
            done[s, i] = now + B_TO_C + LEN_C
    return now, start


def repeat(place, nb, subs):
    keys = [(t + u * 2 * STEPS * nb, kind, s + u * STEPS, i) for u in range(subs) for (kind, s, i), t in place.items()]
    return [k[1:] for k in sorted(keys)]


def find_places(nb, tries, seed):
    place = {}
    for n in range(STEPS * nb):
        s, i = n // nb, nb - 1 - n % nb
        place[0, s, i], place[1, s, i] = 2.0 * n, 2.0 * n + 3.0
    rnd = random.Random(seed)
    names = list(place)
    cur = best = place
    length = low = play(repeat(place, nb, 5), nb)[0]
    for it in range(tries):
        new = dict(cur)
        new[rnd.choice(names)] += rnd.choice((-4.5, -3.5, -2.5, -1.5, 1.5, 2.5, 3.5, 4.5)) + rnd.uniform(-0.2, 0.2)
        played = play(repeat(new, nb, 5), nb)
        if played is None:
            continue
        temp = 60 * (1 - it / tries) + 0.5
        if played[0] <= length or rnd.random() < math.exp((length - played[0]) / temp):
            cur, length = new, played[0]
            if length < low:
                best, low = new, length
    return best


def make_order(place, nb, subs):
    start = play(repeat(place, nb, subs), nb)[1]
    events = [(t, 1, "AB"[key[0]], *key[1:]) for key, t in start.items()]
    events += [(t + LEN_B + B_TO_C, 0, "C", *key[1:]) for key, t in start.items() if key[0] == 1]
    return [e[2:] for e in sorted(events)]


def dot(a, b):
    return jnp.dot(a, b, preferred_element_type=F32)


def dot_nt(a, b):
    return lax.dot_general(a, b, (((1,), (1,)), ((), ())), preferred_element_type=F32)


def kernel(nb, rank, base_eta, lr_in, rate, mask, ut_in, vt_in, ut_out, vt_out,
           r_all, m_all, r_own, m_own, hop_1, ut_land, vt_land, u32, v32, ub, utb, vb,
           rl_sem, ml_sem, r_sem, s_sem, u_sem, v_sem, us_sem, vs_sem, ou_sem, ov_sem, ous_sem, ovs_sem,
           lr, lr_sem, h1_sem, h1s_sem, h2s_sem, h3_sem):
    me = lax.axis_index("blk")
    rep = lax.axis_index("rep")
    other = 1 - rep
    lead = 2 * rep + 1
    mate = 2 * rep
    far_0 = lax.rem(lead + 1, nb)
    far_1 = lax.rem(lead + 2, nb)
    late = nb - 2
    direct = [w for w in range(nb) if w != late]
    parts = hop_1.shape[1]
    rows, cols = r_all.shape[2:]
    subs = lr.shape[1]
    half = cols // 2
    halves = [slice(h * half, (h + 1) * half) for h in range(2)]
    barrier = pltpu.get_barrier_semaphore()

    loads = []
    for w in range(nb):
        start = pl.multiple_of(lax.rem(me + w, nb) * rows, rows)
        loads.append((
            pltpu.make_async_copy(rate.at[pl.ds(start, rows)], r_own.at[w], rl_sem.at[w]),
            pltpu.make_async_copy(mask.at[pl.ds(start, rows)], m_own.at[w], ml_sem.at[w]),
        ))
    for pair in loads:
        for cp in pair:
            cp.start()

    def device(r, b):
        return dict(device_id={"rep": r, "blk": b}, device_id_type=MESH_ID)

    def tell(*who):
        for r, b in who:
            pl.semaphore_signal(barrier, inc=1, **device(r, b))

    def encode(w):
        for cp in loads[w]:
            cp.wait()
        r_own[w] = jnp.where(m_own[w] != 0, r_own[w], jnp.inf)

    def send_factors():
        cps = [
            pltpu.make_async_remote_copy(ut_in, ut_land.at[me], us_sem, u_sem.at[me], **device(rep, lead)),
            pltpu.make_async_remote_copy(vt_in, vt_land.at[me], vs_sem, v_sem.at[me], **device(rep, lead)),
        ]
        for cp in cps:
            cp.start()
        return cps

    def send_block(w):
        cp = pltpu.make_async_remote_copy(
            r_own.at[w], r_all.at[w, me], s_sem.at[w], r_sem.at[w, me], **device(rep, lead)
        )
        cp.start()
        return cp

    def get_results():
        pltpu.make_async_copy(ut_out, ut_out, ou_sem).wait()
        pltpu.make_async_copy(vt_out, vt_out, ov_sem).wait()

    def finish(cps):
        for cp in cps:
            cp.wait_send()
        get_results()

    def part_rows(c):
        return pl.ds(c * hop_1.shape[2], hop_1.shape[2])

    def send_far(side):
        cps = send_factors()
        cps.append(send_block(0))
        for c in range(parts):
            cps.append(pltpu.make_async_remote_copy(
                r_own.at[late, part_rows(c)], hop_1.at[side, c], h1s_sem.at[c], h1_sem.at[side, c],
                **device(other, 2 * other),
            ))
            cps[-1].start()
        for w in direct[1:]:
            encode(w)
        for w in direct[1:]:
            cps.append(send_block(w))
        return cps

    @pl.when(me == far_0)
    def _():
        tell((rep, lead))
        encode(0)
        encode(late)
        pl.semaphore_wait(barrier, 2)
        finish(send_far(0))

    @pl.when(me == far_1)
    def _():
        tell((rep, lead))
        encode(0)
        encode(late)
        pl.semaphore_wait(barrier, 2)
        finish(send_far(1))

    @pl.when(me == mate)
    def _():
        tell((rep, lead), (other, lax.rem(2 * other + 2, nb)), (other, lax.rem(2 * other + 3, nb)))
        encode(0)
        encode(1)
        pl.semaphore_wait(barrier, 2)
        cps = send_factors()
        cps.append(send_block(0))
        for w in range(2, nb):
            encode(w)
        for w in range(1, nb):
            cps.append(send_block(w))
        for c in range(parts):
            for side in range(2):
                pltpu.make_async_copy(hop_1.at[side, c], hop_1.at[side, c], h1_sem.at[side, c]).wait()
                home = lax.rem(2 * other + 2 + side, nb)
                cps.append(pltpu.make_async_remote_copy(
                    hop_1.at[side, c], r_all.at[late, home, part_rows(c)], h2s_sem.at[side, c], h3_sem.at[side, c],
                    **device(other, 2 * other + 1),
                ))
                cps[-1].start()
        finish(cps)

    @pl.when(me == lead)
    def _():
        tell((rep, mate), (rep, far_0), (rep, far_1), (other, 2 * other))
        own = [
            pltpu.make_async_copy(ut_in, ut_land.at[lead], us_sem),
            pltpu.make_async_copy(vt_in, vt_land.at[lead], vs_sem),
            pltpu.make_async_copy(lr_in, lr, lr_sem),
        ]
        for cp in own:
            cp.start()
        for w in range(nb):
            for cp in loads[w]:
                cp.wait()
            m_all[w, lead] = m_own[w].astype(F32).astype(BF16)
            r_all[w, lead] = r_own[w]
        for cp in own:
            cp.wait()
        pl.semaphore_wait(barrier, nb - 1)

        for b in (mate, far_0, far_1):
            pltpu.make_async_copy(ut_land.at[b], ut_land.at[b], u_sem.at[b]).wait()
            pltpu.make_async_copy(vt_land.at[b], vt_land.at[b], v_sem.at[b]).wait()
        for i in range(nb):
            v32[i] = jnp.zeros(v32.shape[1:], F32)
            v32[i, :rank] = vt_land[i]
            vb[i] = v32[i].astype(BF16)
            ut = jnp.concatenate([ut_land[i], jnp.zeros((rows - rank, rows), F32)], axis=0)
            u32[i] = ut.T[:, :KPAD]
            ub[i] = ut.T[:, :KPAD].astype(BF16)
            utb[i] = ut[:KPAD].astype(BF16)

        def run(order, t0, w_of, j_of):
            prod, grads = {}, {}
            for kind, s, i in order:
                sub = s // STEPS
                j, w = j_of(sub, i), w_of(sub)
                if kind == "A":
                    prod[s, i] = [dot(ub[i], vb[j, :, h]) for h in halves]
                elif kind == "B":
                    errs = [
                        (a - r_all[w, j, :, h]).astype(BF16) * m_all[w, j, :, h]
                        for a, h in zip(prod.pop((s, i)), halves)
                    ]
                    gu = [dot_nt(err, vb[j, :, h]) for err, h in zip(errs, halves)]
                    grads[s, i] = gu, [dot(utb[i], err) for err in errs]
                else:
                    eta = lr[s % STEPS, t0 + sub] * base_eta
                    keep = 1.0 - eta * LAMBDA
                    gu, gv = grads.pop((s, i))
                    u_new = u32[i] * keep - eta * gu[0] - eta * gu[1]
                    u32[i] = u_new
                    u_bf = u_new.astype(BF16)
                    ub[i] = u_bf
                    utb[i] = u_bf.T
                    for g, h in zip(gv, halves):
                        v_new = v32[j, :, h] * keep - eta * g
                        v32[j, :, h] = v_new
                        vb[j, :, h] = v_new.astype(BF16)

        place = find_places(nb, 12000, 1)
        order_1 = make_order(place, nb, 1)
        order_n = make_order(place, nb, UNROLL)

        def first_epoch(w, carry):
            pltpu.make_async_copy(r_all.at[w, mate], r_all.at[w, mate], r_sem.at[w, mate]).wait()

            @pl.when(w != late)
            def _():
                for j in (far_0, far_1):
                    pltpu.make_async_copy(r_all.at[w, j], r_all.at[w, j], r_sem.at[w, j]).wait()

            @pl.when(w == late)
            def _():
                for c in range(parts):
                    for side, j in enumerate((far_0, far_1)):
                        dst = r_all.at[late, j, part_rows(c)]
                        pltpu.make_async_copy(dst, dst, h3_sem.at[side, c]).wait()

            for j in (mate, far_0, far_1):
                coded = r_all[w, j]
                seen = coded < jnp.inf
                m_all[w, j] = jnp.where(seen, 1.0, 0.0).astype(BF16)
                r_all[w, j] = jnp.where(seen, coded, 0.0)
            run(order_1, w, lambda sub: w, lambda sub, i: lax.rem(i - w + nb, nb))
            return carry

        def later(n, carry):
            run(order_n, nb + n * UNROLL, lambda sub: sub % nb, lambda sub, i: (i - sub) % nb)
            return carry

        lax.fori_loop(0, nb, first_epoch, 0)
        lax.fori_loop(0, (subs - nb) // UNROLL, later, 0)

        def stage(j):
            vt_land[j] = v32[j, :rank]
            ut_land[j] = jnp.concatenate([u32[j], jnp.zeros((rows, rows - KPAD), F32)], axis=1).T[:rank]

        def send_home(n, j):
            for src, dst, s_out, s_in in ((vt_land, vt_out, ovs_sem, ov_sem), (ut_land, ut_out, ous_sem, ou_sem)):
                cps.append(pltpu.make_async_remote_copy(src.at[j], dst, s_out.at[n], s_in, **device(rep, j)))
                cps[-1].start()

        cps = []
        stage(far_0)
        stage(far_1)
        send_home(0, far_0)
        send_home(1, far_1)
        stage(mate)
        vt_out[...] = v32[lead, :rank]
        send_home(2, mate)
        ut_out[...] = jnp.concatenate([u32[lead], jnp.zeros((rows, rows - KPAD), F32)], axis=1).T[:rank]
        for cp in cps:
            cp.wait_send()


def solution(mesh):
    nb = mesh.shape["blk"]

    def local_run(rate_loc, mask_loc, user_loc, item_loc, lr_scale):
        rows, rank = user_loc.shape
        cols = item_loc.shape[0]
        subs = lr_scale.shape[0]
        base_eta = math.sqrt(rank) / (4.0 * (cols + 2 * rank))
        anywhere = pl.BlockSpec(memory_space=pl.ANY)
        dma = pltpu.SemaphoreType.DMA
        ut, vt = pl.pallas_call(
            functools.partial(kernel, nb, rank, base_eta),
            out_shape=(pltpu.VMEM((rank, rows), F32), pltpu.VMEM((rank, cols), F32)),
            in_specs=[anywhere] * 5,
            out_specs=(pl.BlockSpec(memory_space=pltpu.VMEM),) * 2,
            scratch_shapes=[
                pltpu.VMEM((nb, nb, rows, cols), F32),
                pltpu.VMEM((nb, nb, rows, cols), BF16),
                pltpu.VMEM((nb, rows, cols), F32),
                pltpu.VMEM((nb, rows, cols), jnp.int32),
                pltpu.VMEM((2, 4, rows // 4, cols), F32),
                pltpu.VMEM((nb, rank, rows), F32),
                pltpu.VMEM((nb, rank, cols), F32),
                pltpu.VMEM((nb, rows, KPAD), F32),
                pltpu.VMEM((nb, KPAD, cols), F32),
                pltpu.VMEM((nb, rows, KPAD), BF16),
                pltpu.VMEM((nb, KPAD, rows), BF16),
                pltpu.VMEM((nb, KPAD, cols), BF16),
                dma((nb,)), dma((nb,)),
                dma((nb, nb)), dma((nb,)), dma((nb,)), dma((nb,)), dma, dma,
                dma, dma, dma((nb - 1,)), dma((nb - 1,)),
                pltpu.SMEM((STEPS, subs), F32), dma,
                dma((2, 4)), dma((4,)), dma((2, 4)), dma((2, 4)),
            ],
            compiler_params=pltpu.CompilerParams(collective_id=0, has_side_effects=True),
            name="dsgd",
        )(lr_scale.T, rate_loc, mask_loc, user_loc.T, item_loc.T)
        return ut.T, vt.T

    spec_cols = P(None, ("rep", "blk"))
    spec_rows = P(("rep", "blk"), None)
    return jax.shard_map(
        local_run,
        mesh=mesh,
        in_specs=(spec_cols, spec_cols, spec_rows, spec_rows, P(None, None)),
        out_specs=(spec_rows, spec_rows),
        check_vma=False,
    )
```

```python
import functools
import math
import random

import jax
import jax.numpy as jnp
from jax import lax
from jax.experimental import pallas as pl
from jax.experimental.pallas import tpu as pltpu
from jax.sharding import PartitionSpec as P

LAMBDA = 0.05
STEPS = 4
KPAD = 64
UNROLL = 12
LEN_A, LEN_B, A_TO_B, B_TO_C, LEN_C = 64, 96, 226, 211, 35
F32 = jnp.float32
BF16 = jnp.bfloat16
MESH_ID = pl.DeviceIdType.MESH


def play(order, nb):
    now, start, done = 0, {}, {}
    for kind, s, i in order:
        if kind == 0:
            ready = 0
            if s > 0:
                before = [(s - 1, i)] + ([(s - 1, (i - 1) % nb)] if s % STEPS == 0 else [])
                if any(d not in done for d in before):
                    return None
                ready = max(done[d] for d in before)
            now = max(now, ready)
            start[kind, s, i] = now
            now += LEN_A
        else:
            if (0, s, i) not in start:
                return None
            now = max(now, start[0, s, i] + A_TO_B)
            start[kind, s, i] = now
            now += LEN_B
            done[s, i] = now + B_TO_C + LEN_C
    return now, start


def repeat(place, nb, subs):
    keys = [(t + u * 2 * STEPS * nb, kind, s + u * STEPS, i) for u in range(subs) for (kind, s, i), t in place.items()]
    return [k[1:] for k in sorted(keys)]


def find_places(nb, tries, seed):
    place = {}
    for n in range(STEPS * nb):
        s, i = n // nb, nb - 1 - n % nb
        place[0, s, i], place[1, s, i] = 2.0 * n, 2.0 * n + 3.0
    rnd = random.Random(seed)
    names = list(place)
    cur = best = place
    length = low = play(repeat(place, nb, 5), nb)[0]
    for it in range(tries):
        new = dict(cur)
        new[rnd.choice(names)] += rnd.choice((-4.5, -3.5, -2.5, -1.5, 1.5, 2.5, 3.5, 4.5)) + rnd.uniform(-0.2, 0.2)
        played = play(repeat(new, nb, 5), nb)
        if played is None:
            continue
        temp = 60 * (1 - it / tries) + 0.5
        if played[0] <= length or rnd.random() < math.exp((length - played[0]) / temp):
            cur, length = new, played[0]
            if length < low:
                best, low = new, length
    return best


def make_order(place, nb, subs):
    start = play(repeat(place, nb, subs), nb)[1]
    events = [(t, 1, "AB"[key[0]], *key[1:]) for key, t in start.items()]
    events += [(t + LEN_B + B_TO_C, 0, "C", *key[1:]) for key, t in start.items() if key[0] == 1]
    return [e[2:] for e in sorted(events)]


def dot(a, b):
    return jnp.dot(a, b, preferred_element_type=F32)


def dot_nt(a, b):
    return lax.dot_general(a, b, (((1,), (1,)), ((), ())), preferred_element_type=F32)


def kernel(nb, rank, base_eta, lr_in, rate, mask, ut_in, vt_in, ut_out, vt_out,
           r_all, m_all, r_own, m_own, hop_1, ut_land, vt_land, u32, v32, ub, utb, vb,
           rl_sem, ml_sem, r_sem, s_sem, u_sem, v_sem, us_sem, vs_sem, ou_sem, ov_sem, ous_sem, ovs_sem,
           lr, lr_sem, h1_sem, h1s_sem, h2s_sem, h3_sem):
    me = lax.axis_index("blk")
    rep = lax.axis_index("rep")
    other = 1 - rep
    lead = 2 * rep + 1
    mate = 2 * rep
    far_0 = lax.rem(lead + 1, nb)
    far_1 = lax.rem(lead + 2, nb)
    late = nb - 2
    last = nb - 1
    depth = hop_1.shape[2]
    pieces = [(late, c) for c in range(r_all.shape[2] // depth)] + [(last, 0)]
    rest = pl.ds(depth, r_all.shape[2] - depth)
    rows, cols = r_all.shape[2:]
    subs = lr.shape[1]
    half = cols // 2
    halves = [slice(h * half, (h + 1) * half) for h in range(2)]
    barrier = pltpu.get_barrier_semaphore()

    loads = []
    for w in range(nb):
        start = pl.multiple_of(lax.rem(me + w, nb) * rows, rows)
        loads.append((
            pltpu.make_async_copy(rate.at[pl.ds(start, rows)], r_own.at[w], rl_sem.at[w]),
            pltpu.make_async_copy(mask.at[pl.ds(start, rows)], m_own.at[w], ml_sem.at[w]),
        ))
    for pair in loads:
        for cp in pair:
            cp.start()

    def device(r, b):
        return dict(device_id={"rep": r, "blk": b}, device_id_type=MESH_ID)

    def tell(*who):
        for r, b in who:
            pl.semaphore_signal(barrier, inc=1, **device(r, b))

    def encode(w):
        for cp in loads[w]:
            cp.wait()
        r_own[w] = jnp.where(m_own[w] != 0, r_own[w], jnp.inf)

    def send_factors():
        cps = [
            pltpu.make_async_remote_copy(ut_in, ut_land.at[me], us_sem, u_sem.at[me], **device(rep, lead)),
            pltpu.make_async_remote_copy(vt_in, vt_land.at[me], vs_sem, v_sem.at[me], **device(rep, lead)),
        ]
        for cp in cps:
            cp.start()
        return cps

    def send_block(w):
        cp = pltpu.make_async_remote_copy(
            r_own.at[w], r_all.at[w, me], s_sem.at[w], r_sem.at[w, me], **device(rep, lead)
        )
        cp.start()
        return cp

    def get_results():
        pltpu.make_async_copy(ut_out, ut_out, ou_sem).wait()
        pltpu.make_async_copy(vt_out, vt_out, ov_sem).wait()

    def finish(cps):
        for cp in cps:
            cp.wait_send()
        get_results()

    def part_rows(c):
        return pl.ds(c * depth, depth)

    def send_far(side):
        cps = send_factors()
        cps.append(send_block(0))
        for n, (w, c) in enumerate(pieces):
            if c == 0:
                encode(w)
            cps.append(pltpu.make_async_remote_copy(
                r_own.at[w, part_rows(c)], hop_1.at[side, n], h1s_sem.at[n], h1_sem.at[side, n],
                **device(other, 2 * other),
            ))
            cps[-1].start()
        for w in range(1, late):
            encode(w)
            cps.append(send_block(w))
        cps.append(pltpu.make_async_remote_copy(
            r_own.at[last, rest], r_all.at[last, me, rest], s_sem.at[last], r_sem.at[last, me], **device(rep, lead)
        ))
        cps[-1].start()
        return cps

    @pl.when(me == far_0)
    def _():
        tell((rep, lead))
        encode(0)
        pl.semaphore_wait(barrier, 2)
        finish(send_far(0))

    @pl.when(me == far_1)
    def _():
        tell((rep, lead))
        encode(0)
        pl.semaphore_wait(barrier, 2)
        finish(send_far(1))

    @pl.when(me == mate)
    def _():
        tell((rep, lead), (other, lax.rem(2 * other + 2, nb)), (other, lax.rem(2 * other + 3, nb)))
        encode(0)
        encode(1)
        pl.semaphore_wait(barrier, 2)
        cps = send_factors()
        cps.append(send_block(0))
        for w in range(2, nb):
            encode(w)
        for w in range(1, nb):
            cps.append(send_block(w))
        for n, (w, c) in enumerate(pieces):
            for side in range(2):
                pltpu.make_async_copy(hop_1.at[side, n], hop_1.at[side, n], h1_sem.at[side, n]).wait()
                home = lax.rem(2 * other + 2 + side, nb)
                cps.append(pltpu.make_async_remote_copy(
                    hop_1.at[side, n], r_all.at[w, home, part_rows(c)], h2s_sem.at[side, n], h3_sem.at[side, n],
                    **device(other, 2 * other + 1),
                ))
                cps[-1].start()
        finish(cps)

    @pl.when(me == lead)
    def _():
        tell((rep, mate), (rep, far_0), (rep, far_1), (other, 2 * other))
        own = [
            pltpu.make_async_copy(ut_in, ut_land.at[lead], us_sem),
            pltpu.make_async_copy(vt_in, vt_land.at[lead], vs_sem),
            pltpu.make_async_copy(lr_in, lr, lr_sem),
        ]
        for cp in own:
            cp.start()
        for w in range(nb):
            for cp in loads[w]:
                cp.wait()
            m_all[w, lead] = m_own[w].astype(F32).astype(BF16)
            r_all[w, lead] = r_own[w]
        for cp in own:
            cp.wait()
        pl.semaphore_wait(barrier, nb - 1)

        for b in (mate, far_0, far_1):
            pltpu.make_async_copy(ut_land.at[b], ut_land.at[b], u_sem.at[b]).wait()
            pltpu.make_async_copy(vt_land.at[b], vt_land.at[b], v_sem.at[b]).wait()
        for i in range(nb):
            v32[i] = jnp.zeros(v32.shape[1:], F32)
            v32[i, :rank] = vt_land[i]
            vb[i] = v32[i].astype(BF16)
            ut = jnp.concatenate([ut_land[i], jnp.zeros((rows - rank, rows), F32)], axis=0)
            u32[i] = ut.T[:, :KPAD]
            ub[i] = ut.T[:, :KPAD].astype(BF16)
            utb[i] = ut[:KPAD].astype(BF16)

        def run(order, t0, w_of, j_of):
            prod, grads = {}, {}
            for kind, s, i in order:
                sub = s // STEPS
                j, w = j_of(sub, i), w_of(sub)
                if kind == "A":
                    prod[s, i] = [dot(ub[i], vb[j, :, h]) for h in halves]
                elif kind == "B":
                    errs = [
                        (a - r_all[w, j, :, h]).astype(BF16) * m_all[w, j, :, h]
                        for a, h in zip(prod.pop((s, i)), halves)
                    ]
                    gu = [dot_nt(err, vb[j, :, h]) for err, h in zip(errs, halves)]
                    grads[s, i] = gu, [dot(utb[i], err) for err in errs]
                else:
                    eta = lr[s % STEPS, t0 + sub] * base_eta
                    keep = 1.0 - eta * LAMBDA
                    gu, gv = grads.pop((s, i))
                    u_new = u32[i] * keep - eta * gu[0] - eta * gu[1]
                    u32[i] = u_new
                    u_bf = u_new.astype(BF16)
                    ub[i] = u_bf
                    utb[i] = u_bf.T
                    for g, h in zip(gv, halves):
                        v_new = v32[j, :, h] * keep - eta * g
                        v32[j, :, h] = v_new
                        vb[j, :, h] = v_new.astype(BF16)

        place = find_places(nb, 12000, 1)
        order_1 = make_order(place, nb, 1)
        order_n = make_order(place, nb, UNROLL)

        def first_epoch(w, carry):
            pltpu.make_async_copy(r_all.at[w, mate], r_all.at[w, mate], r_sem.at[w, mate]).wait()

            @pl.when(w < late)
            def _():
                for j in (far_0, far_1):
                    pltpu.make_async_copy(r_all.at[w, j], r_all.at[w, j], r_sem.at[w, j]).wait()

            for row in (late, last):
                @pl.when(w == row)
                def _():
                    for side, j in enumerate((far_0, far_1)):
                        for n, (at, c) in enumerate(pieces):
                            if at == row:
                                dst = r_all.at[row, j, part_rows(c)]
                                pltpu.make_async_copy(dst, dst, h3_sem.at[side, n]).wait()
                        if row == last:
                            dst = r_all.at[last, j, rest]
                            pltpu.make_async_copy(dst, dst, r_sem.at[last, j]).wait()

            for j in (mate, far_0, far_1):
                coded = r_all[w, j]
                seen = coded < jnp.inf
                m_all[w, j] = jnp.where(seen, 1.0, 0.0).astype(BF16)
                r_all[w, j] = jnp.where(seen, coded, 0.0)
            run(order_1, w, lambda sub: w, lambda sub, i: lax.rem(i - w + nb, nb))
            return carry

        def later(n, carry):
            run(order_n, nb + n * UNROLL, lambda sub: sub % nb, lambda sub, i: (i - sub) % nb)
            return carry

        lax.fori_loop(0, nb, first_epoch, 0)
        lax.fori_loop(0, (subs - nb) // UNROLL, later, 0)

        def stage(j):
            vt_land[j] = v32[j, :rank]
            ut_land[j] = jnp.concatenate([u32[j], jnp.zeros((rows, rows - KPAD), F32)], axis=1).T[:rank]

        def send_home(n, j):
            for src, dst, s_out, s_in in ((vt_land, vt_out, ovs_sem, ov_sem), (ut_land, ut_out, ous_sem, ou_sem)):
                cps.append(pltpu.make_async_remote_copy(src.at[j], dst, s_out.at[n], s_in, **device(rep, j)))
                cps[-1].start()

        cps = []
        stage(far_0)
        stage(far_1)
        send_home(0, far_0)
        send_home(1, far_1)
        stage(mate)
        vt_out[...] = v32[lead, :rank]
        send_home(2, mate)
        ut_out[...] = jnp.concatenate([u32[lead], jnp.zeros((rows, rows - KPAD), F32)], axis=1).T[:rank]
        for cp in cps:
            cp.wait_send()


def solution(mesh):
    nb = mesh.shape["blk"]

    def local_run(rate_loc, mask_loc, user_loc, item_loc, lr_scale):
        rows, rank = user_loc.shape
        cols = item_loc.shape[0]
        subs = lr_scale.shape[0]
        base_eta = math.sqrt(rank) / (4.0 * (cols + 2 * rank))
        anywhere = pl.BlockSpec(memory_space=pl.ANY)
        dma = pltpu.SemaphoreType.DMA
        ut, vt = pl.pallas_call(
            functools.partial(kernel, nb, rank, base_eta),
            out_shape=(pltpu.VMEM((rank, rows), F32), pltpu.VMEM((rank, cols), F32)),
            in_specs=[anywhere] * 5,
            out_specs=(pl.BlockSpec(memory_space=pltpu.VMEM),) * 2,
            scratch_shapes=[
                pltpu.VMEM((nb, nb, rows, cols), F32),
                pltpu.VMEM((nb, nb, rows, cols), BF16),
                pltpu.VMEM((nb, rows, cols), F32),
                pltpu.VMEM((nb, rows, cols), jnp.int32),
                pltpu.VMEM((2, 5, rows // 4, cols), F32),
                pltpu.VMEM((nb, rank, rows), F32),
                pltpu.VMEM((nb, rank, cols), F32),
                pltpu.VMEM((nb, rows, KPAD), F32),
                pltpu.VMEM((nb, KPAD, cols), F32),
                pltpu.VMEM((nb, rows, KPAD), BF16),
                pltpu.VMEM((nb, KPAD, rows), BF16),
                pltpu.VMEM((nb, KPAD, cols), BF16),
                dma((nb,)), dma((nb,)),
                dma((nb, nb)), dma((nb,)), dma((nb,)), dma((nb,)), dma, dma,
                dma, dma, dma((nb - 1,)), dma((nb - 1,)),
                pltpu.SMEM((STEPS, subs), F32), dma,
                dma((2, 5)), dma((5,)), dma((2, 5)), dma((2, 5)),
            ],
            compiler_params=pltpu.CompilerParams(collective_id=0, has_side_effects=True),
            name="dsgd",
        )(lr_scale.T, rate_loc, mask_loc, user_loc.T, item_loc.T)
        return ut.T, vt.T

    spec_cols = P(None, ("rep", "blk"))
    spec_rows = P(("rep", "blk"), None)
    return jax.shard_map(
        local_run,
        mesh=mesh,
        in_specs=(spec_cols, spec_cols, spec_rows, spec_rows, P(None, None)),
        out_specs=(spec_rows, spec_rows),
        check_vma=False,
    )
```

```python
import functools
import math
import random

import jax
import jax.numpy as jnp
from jax import lax
from jax.experimental import pallas as pl
from jax.experimental.pallas import tpu as pltpu
from jax.sharding import PartitionSpec as P

LAMBDA = 0.05
STEPS = 4
KPAD = 64
UNROLL = 20
LEN_A, LEN_B, A_TO_B, B_TO_C, LEN_C = 64, 96, 226, 211, 35
F32 = jnp.float32
BF16 = jnp.bfloat16
MESH_ID = pl.DeviceIdType.MESH


def play(order, nb):
    now, start, done = 0, {}, {}
    for kind, s, i in order:
        if kind == 0:
            ready = 0
            if s > 0:
                before = [(s - 1, i)] + ([(s - 1, (i - 1) % nb)] if s % STEPS == 0 else [])
                if any(d not in done for d in before):
                    return None
                ready = max(done[d] for d in before)
            now = max(now, ready)
            start[kind, s, i] = now
            now += LEN_A
        else:
            if (0, s, i) not in start:
                return None
            now = max(now, start[0, s, i] + A_TO_B)
            start[kind, s, i] = now
            now += LEN_B
            done[s, i] = now + B_TO_C + LEN_C
    return now, start


def repeat(place, nb, subs):
    keys = [(t + u * 2 * STEPS * nb, kind, s + u * STEPS, i) for u in range(subs) for (kind, s, i), t in place.items()]
    return [k[1:] for k in sorted(keys)]


def find_places(nb, tries, seed):
    place = {}
    for n in range(STEPS * nb):
        s, i = n // nb, nb - 1 - n % nb
        place[0, s, i], place[1, s, i] = 2.0 * n, 2.0 * n + 3.0
    rnd = random.Random(seed)
    names = list(place)
    cur = best = place
    length = low = play(repeat(place, nb, 5), nb)[0]
    for it in range(tries):
        new = dict(cur)
        new[rnd.choice(names)] += rnd.choice((-4.5, -3.5, -2.5, -1.5, 1.5, 2.5, 3.5, 4.5)) + rnd.uniform(-0.2, 0.2)
        played = play(repeat(new, nb, 5), nb)
        if played is None:
            continue
        temp = 60 * (1 - it / tries) + 0.5
        if played[0] <= length or rnd.random() < math.exp((length - played[0]) / temp):
            cur, length = new, played[0]
            if length < low:
                best, low = new, length
    return best


def make_order(place, nb, subs):
    start = play(repeat(place, nb, subs), nb)[1]
    events = [(t, 1, "AB"[key[0]], *key[1:]) for key, t in start.items()]
    events += [(t + LEN_B + B_TO_C, 0, "C", *key[1:]) for key, t in start.items() if key[0] == 1]
    return [e[2:] for e in sorted(events)]


def dot(a, b):
    return jnp.dot(a, b, preferred_element_type=F32)


def dot_nt(a, b):
    return lax.dot_general(a, b, (((1,), (1,)), ((), ())), preferred_element_type=F32)


def kernel(nb, rank, base_eta, lr_in, rate, mask, ut_in, vt_in, ut_out, vt_out,
           r_all, m_all, r_own, m_own, hop_1, ut_land, vt_land, u32, v32, ub, utb, vb,
           rl_sem, ml_sem, r_sem, s_sem, u_sem, v_sem, us_sem, vs_sem, ou_sem, ov_sem, ous_sem, ovs_sem,
           lr, lr_sem, h1_sem, h1s_sem, h2s_sem, h3_sem):
    me = lax.axis_index("blk")
    rep = lax.axis_index("rep")
    other = 1 - rep
    lead = 2 * rep + 1
    mate = 2 * rep
    far_0 = lax.rem(lead + 1, nb)
    far_1 = lax.rem(lead + 2, nb)
    late = nb - 2
    last = nb - 1
    depth = hop_1.shape[2]
    pieces = [(late, c) for c in range(r_all.shape[2] // depth)] + [(last, 0)]
    rest = pl.ds(depth, r_all.shape[2] - depth)
    rows, cols = r_all.shape[2:]
    subs = lr.shape[1]
    half = cols // 2
    halves = [slice(h * half, (h + 1) * half) for h in range(2)]
    barrier = pltpu.get_barrier_semaphore()

    loads = []
    for w in range(nb):
        start = pl.multiple_of(lax.rem(me + w, nb) * rows, rows)
        loads.append((
            pltpu.make_async_copy(rate.at[pl.ds(start, rows)], r_own.at[w], rl_sem.at[w]),
            pltpu.make_async_copy(mask.at[pl.ds(start, rows)], m_own.at[w], ml_sem.at[w]),
        ))
    for pair in loads:
        for cp in pair:
            cp.start()

    def device(r, b):
        return dict(device_id={"rep": r, "blk": b}, device_id_type=MESH_ID)

    def tell(*who):
        for r, b in who:
            pl.semaphore_signal(barrier, inc=1, **device(r, b))

    def encode(w):
        for cp in loads[w]:
            cp.wait()
        r_own[w] = jnp.where(m_own[w] != 0, r_own[w], jnp.inf)

    def send_factors():
        cps = [
            pltpu.make_async_remote_copy(ut_in, ut_land.at[me], us_sem, u_sem.at[me], **device(rep, lead)),
            pltpu.make_async_remote_copy(vt_in, vt_land.at[me], vs_sem, v_sem.at[me], **device(rep, lead)),
        ]
        for cp in cps:
            cp.start()
        return cps

    def send_block(w):
        cp = pltpu.make_async_remote_copy(
            r_own.at[w], r_all.at[w, me], s_sem.at[w], r_sem.at[w, me], **device(rep, lead)
        )
        cp.start()
        return cp

    def get_results():
        pltpu.make_async_copy(ut_out, ut_out, ou_sem).wait()
        pltpu.make_async_copy(vt_out, vt_out, ov_sem).wait()

    def finish(cps):
        for cp in cps:
            cp.wait_send()
        get_results()

    def part_rows(c):
        return pl.ds(c * depth, depth)

    def send_far(side):
        cps = send_factors()
        cps.append(send_block(0))
        for n, (w, c) in enumerate(pieces):
            if c == 0:
                encode(w)
            cps.append(pltpu.make_async_remote_copy(
                r_own.at[w, part_rows(c)], hop_1.at[side, n], h1s_sem.at[n], h1_sem.at[side, n],
                **device(other, 2 * other),
            ))
            cps[-1].start()
        for w in range(1, late):
            encode(w)
            cps.append(send_block(w))
        cps.append(pltpu.make_async_remote_copy(
            r_own.at[last, rest], r_all.at[last, me, rest], s_sem.at[last], r_sem.at[last, me], **device(rep, lead)
        ))
        cps[-1].start()
        return cps

    @pl.when(me == far_0)
    def _():
        tell((rep, lead))
        encode(0)
        pl.semaphore_wait(barrier, 2)
        finish(send_far(0))

    @pl.when(me == far_1)
    def _():
        tell((rep, lead))
        encode(0)
        pl.semaphore_wait(barrier, 2)
        finish(send_far(1))

    @pl.when(me == mate)
    def _():
        tell((rep, lead), (other, lax.rem(2 * other + 2, nb)), (other, lax.rem(2 * other + 3, nb)))
        encode(0)
        encode(1)
        pl.semaphore_wait(barrier, 2)
        cps = send_factors()
        cps.append(send_block(0))
        for w in range(2, nb):
            encode(w)
        for w in range(1, nb):
            cps.append(send_block(w))
        for n, (w, c) in enumerate(pieces):
            for side in range(2):
                pltpu.make_async_copy(hop_1.at[side, n], hop_1.at[side, n], h1_sem.at[side, n]).wait()
                home = lax.rem(2 * other + 2 + side, nb)
                cps.append(pltpu.make_async_remote_copy(
                    hop_1.at[side, n], r_all.at[w, home, part_rows(c)], h2s_sem.at[side, n], h3_sem.at[side, n],
                    **device(other, 2 * other + 1),
                ))
                cps[-1].start()
        finish(cps)

    @pl.when(me == lead)
    def _():
        tell((rep, mate), (rep, far_0), (rep, far_1), (other, 2 * other))
        own = [
            pltpu.make_async_copy(ut_in, ut_land.at[lead], us_sem),
            pltpu.make_async_copy(vt_in, vt_land.at[lead], vs_sem),
            pltpu.make_async_copy(lr_in, lr, lr_sem),
        ]
        for cp in own:
            cp.start()
        for w in range(nb):
            for cp in loads[w]:
                cp.wait()
            m_all[w, lead] = m_own[w].astype(F32).astype(BF16)
            r_all[w, lead] = r_own[w]
        for cp in own:
            cp.wait()
        pl.semaphore_wait(barrier, nb - 1)

        for b in (mate, far_0, far_1):
            pltpu.make_async_copy(ut_land.at[b], ut_land.at[b], u_sem.at[b]).wait()
            pltpu.make_async_copy(vt_land.at[b], vt_land.at[b], v_sem.at[b]).wait()
        for i in range(nb):
            v32[i] = jnp.zeros(v32.shape[1:], F32)
            v32[i, :rank] = vt_land[i]
            vb[i] = v32[i].astype(BF16)
            ut = jnp.concatenate([ut_land[i], jnp.zeros((rows - rank, rows), F32)], axis=0)
            u32[i] = ut.T[:, :KPAD]
            ub[i] = ut.T[:, :KPAD].astype(BF16)
            utb[i] = ut[:KPAD].astype(BF16)

        def run(order, t0, w_of, j_of):
            prod, grads = {}, {}
            for kind, s, i in order:
                sub = s // STEPS
                j, w = j_of(sub, i), w_of(sub)
                if kind == "A":
                    prod[s, i] = [dot(ub[i], vb[j, :, h]) for h in halves]
                elif kind == "B":
                    errs = [
                        (a - r_all[w, j, :, h]).astype(BF16) * m_all[w, j, :, h]
                        for a, h in zip(prod.pop((s, i)), halves)
                    ]
                    gu = [dot_nt(err, vb[j, :, h]) for err, h in zip(errs, halves)]
                    grads[s, i] = gu, [dot(utb[i], err) for err in errs]
                else:
                    eta = lr[s % STEPS, t0 + sub] * base_eta
                    keep = 1.0 - eta * LAMBDA
                    gu, gv = grads.pop((s, i))
                    u_new = u32[i] * keep - eta * gu[0] - eta * gu[1]
                    u32[i] = u_new
                    u_bf = u_new.astype(BF16)
                    ub[i] = u_bf
                    utb[i] = u_bf.T
                    for g, h in zip(gv, halves):
                        v_new = v32[j, :, h] * keep - eta * g
                        v32[j, :, h] = v_new
                        vb[j, :, h] = v_new.astype(BF16)

        place = find_places(nb, 12000, 1)
        order_1 = make_order(place, nb, 1)
        order_n = make_order(place, nb, UNROLL)

        def first_epoch(w, carry):
            pltpu.make_async_copy(r_all.at[w, mate], r_all.at[w, mate], r_sem.at[w, mate]).wait()

            @pl.when(w < late)
            def _():
                for j in (far_0, far_1):
                    pltpu.make_async_copy(r_all.at[w, j], r_all.at[w, j], r_sem.at[w, j]).wait()

            for row in (late, last):
                @pl.when(w == row)
                def _():
                    for side, j in enumerate((far_0, far_1)):
                        for n, (at, c) in enumerate(pieces):
                            if at == row:
                                dst = r_all.at[row, j, part_rows(c)]
                                pltpu.make_async_copy(dst, dst, h3_sem.at[side, n]).wait()
                        if row == last:
                            dst = r_all.at[last, j, rest]
                            pltpu.make_async_copy(dst, dst, r_sem.at[last, j]).wait()

            for j in (mate, far_0, far_1):
                coded = r_all[w, j]
                seen = coded < jnp.inf
                m_all[w, j] = jnp.where(seen, 1.0, 0.0).astype(BF16)
                r_all[w, j] = jnp.where(seen, coded, 0.0)
            run(order_1, w, lambda sub: w, lambda sub, i: lax.rem(i - w + nb, nb))
            return carry

        def later(n, carry):
            run(order_n, nb + n * UNROLL, lambda sub: sub % nb, lambda sub, i: (i - sub) % nb)
            return carry

        lax.fori_loop(0, nb, first_epoch, 0)
        lax.fori_loop(0, (subs - nb) // UNROLL, later, 0)

        def stage(j):
            vt_land[j] = v32[j, :rank]
            ut_land[j] = jnp.concatenate([u32[j], jnp.zeros((rows, rows - KPAD), F32)], axis=1).T[:rank]

        def send_home(n, j):
            for src, dst, s_out, s_in in ((vt_land, vt_out, ovs_sem, ov_sem), (ut_land, ut_out, ous_sem, ou_sem)):
                cps.append(pltpu.make_async_remote_copy(src.at[j], dst, s_out.at[n], s_in, **device(rep, j)))
                cps[-1].start()

        cps = []
        stage(far_0)
        stage(far_1)
        send_home(0, far_0)
        send_home(1, far_1)
        stage(mate)
        vt_out[...] = v32[lead, :rank]
        send_home(2, mate)
        ut_out[...] = jnp.concatenate([u32[lead], jnp.zeros((rows, rows - KPAD), F32)], axis=1).T[:rank]
        for cp in cps:
            cp.wait_send()


def solution(mesh):
    nb = mesh.shape["blk"]

    def local_run(rate_loc, mask_loc, user_loc, item_loc, lr_scale):
        rows, rank = user_loc.shape
        cols = item_loc.shape[0]
        subs = lr_scale.shape[0]
        base_eta = math.sqrt(rank) / (4.0 * (cols + 2 * rank))
        anywhere = pl.BlockSpec(memory_space=pl.ANY)
        dma = pltpu.SemaphoreType.DMA
        ut, vt = pl.pallas_call(
            functools.partial(kernel, nb, rank, base_eta),
            out_shape=(pltpu.VMEM((rank, rows), F32), pltpu.VMEM((rank, cols), F32)),
            in_specs=[anywhere] * 5,
            out_specs=(pl.BlockSpec(memory_space=pltpu.VMEM),) * 2,
            scratch_shapes=[
                pltpu.VMEM((nb, nb, rows, cols), F32),
                pltpu.VMEM((nb, nb, rows, cols), BF16),
                pltpu.VMEM((nb, rows, cols), F32),
                pltpu.VMEM((nb, rows, cols), jnp.int32),
                pltpu.VMEM((2, 5, rows // 4, cols), F32),
                pltpu.VMEM((nb, rank, rows), F32),
                pltpu.VMEM((nb, rank, cols), F32),
                pltpu.VMEM((nb, rows, KPAD), F32),
                pltpu.VMEM((nb, KPAD, cols), F32),
                pltpu.VMEM((nb, rows, KPAD), BF16),
                pltpu.VMEM((nb, KPAD, rows), BF16),
                pltpu.VMEM((nb, KPAD, cols), BF16),
                dma((nb,)), dma((nb,)),
                dma((nb, nb)), dma((nb,)), dma((nb,)), dma((nb,)), dma, dma,
                dma, dma, dma((nb - 1,)), dma((nb - 1,)),
                pltpu.SMEM((STEPS, subs), F32), dma,
                dma((2, 5)), dma((5,)), dma((2, 5)), dma((2, 5)),
            ],
            compiler_params=pltpu.CompilerParams(collective_id=0, has_side_effects=True),
            name="dsgd",
        )(lr_scale.T, rate_loc, mask_loc, user_loc.T, item_loc.T)
        return ut.T, vt.T

    spec_cols = P(None, ("rep", "blk"))
    spec_rows = P(("rep", "blk"), None)
    return jax.shard_map(
        local_run,
        mesh=mesh,
        in_specs=(spec_cols, spec_cols, spec_rows, spec_rows, P(None, None)),
        out_specs=(spec_rows, spec_rows),
        check_vma=False,
    )
```
